32 devices in a mesh: dp: 1 (over z), tp: 4 (over y), ep: 8 (over x, core).
Axes of the slice: x: 4, y: 4, z: 1, core: 2. Of those that a mesh axis runs over, the one named last changes fastest.
The devices are a block of a 4x4x8 slice.
Arguments:
- emb: bfloat16 [2, 256, 2048], P(None, ('dp', 'ep'))
- pos: int32 [256], P(('dp', 'ep'))
- route_ids: int32 [2, 256, 6], P(None, ('dp', 'ep'))
- lat_cache: bfloat16 [2, 256, 128, 512], P(None, ('dp', 'ep'))
- rope_cache: bfloat16 [2, 256, 128, 64], P(None, ('dp', 'ep'))
- attn_norm: float32 [2, 2048], replicated
- w_q: bfloat16 [2, 2048, 16, 192], P(None, None, 'tp')
- w_dkv: bfloat16 [2, 2048, 576], replicated
- kv_norm: float32 [2, 512], replicated
- w_uk: bfloat16 [2, 512, 16, 128], P(None, None, 'tp')
- w_uv: bfloat16 [2, 512, 16, 128], P(None, None, 'tp')
- w_o: bfloat16 [2, 2048, 2048], P(None, 'tp')
- mlp_norm: float32 [2, 2048], replicated
- dense_gate: bfloat16 [2048, 10944], P(None, 'tp')
- dense_up: bfloat16 [2048, 10944], P(None, 'tp')
- dense_down: bfloat16 [10944, 2048], P('tp')
- router: bfloat16 [2048, 64], replicated
- shared_gate: bfloat16 [2048, 2816], P(None, 'tp')
- shared_up: bfloat16 [2048, 2816], P(None, 'tp')
- shared_down: bfloat16 [2816, 2048], P('tp')
- expert_gate: bfloat16 [64, 2048, 1408], P('ep', None, 'tp')
- expert_up: bfloat16 [64, 2048, 1408], P('ep', None, 'tp')
- expert_down: bfloat16 [64, 1408, 2048], P('ep', 'tp')
Outputs:
- output 1: bfloat16 [2, 256, 2048], P(None, ('dp', 'ep'))
- output 2: bfloat16 [2, 256, 128, 512], P(None, ('dp', 'ep'))
- output 3: bfloat16 [2, 256, 128, 64], P(None, ('dp', 'ep'))
All inputs are finite; a program needn't handle non-finite values.
Results may differ from the reference program's by a relative error of at most 0.02.
Values are sent between devices in bfloat16 or wider.
A program may use at most 768 MiB of HBM per device.

```python
import math
import jax
import jax.numpy as jnp
from jax import lax

HIDDEN = 2048
NUM_HEADS = 16
NOPE_DIM = 128
ROPE_DIM = 64
KV_LORA = 512
V_HEAD = 128
DENSE_FF = 10944
EXPERTS = 64
EXPERT_FF = 1408
SHARED_FF = 2816
TOP_K = 6
TOKENS = 256
CACHE_LEN = 128

QK_DIM = NOPE_DIM + ROPE_DIM
SCORE_SCALE = 1.0 / math.sqrt(QK_DIM)
NORM_EPS = 1e-6
ROPE_THETA = 10000.0
ROUTE_SCALE = 1.5 * EXPERTS / TOP_K
LATENT_GAIN = 0.5 * math.log(CACHE_LEN)


def rms_norm(values, gain):
    wide = values.astype(jnp.float32)
    mean_sq = jnp.mean(wide * wide, axis=-1, keepdims=True)
    return (wide * lax.rsqrt(mean_sq + NORM_EPS) * gain).astype(jnp.bfloat16)


def rope_tables(position):
    half_dim = ROPE_DIM // 2
    inv_freq = ROPE_THETA ** (-(jnp.arange(half_dim, dtype=jnp.float32) * 2.0 / ROPE_DIM))
    angles = position.astype(jnp.float32)[:, None] * inv_freq[None, :]
    return jnp.cos(angles), jnp.sin(angles)


def rotary(values, cos_t, sin_t):
    wide = values.astype(jnp.float32)
    half_dim = wide.shape[-1] // 2
    first = wide[..., :half_dim]
    second = wide[..., half_dim:]
    return jnp.concatenate([first * cos_t - second * sin_t, second * cos_t + first * sin_t], axis=-1)


def attention(hidden, cur_pos, lat, rop, g_attn, w_query, w_dkv, g_kv, w_uk, w_uv, w_out):
    tokens = hidden.shape[0]
    cos_t, sin_t = rope_tables(cur_pos)
    normed = rms_norm(hidden, g_attn)
    query = jnp.dot(normed, w_query.reshape(HIDDEN, NUM_HEADS * QK_DIM), preferred_element_type=jnp.float32).reshape(tokens, NUM_HEADS, QK_DIM)
    q_nope = query[..., :NOPE_DIM].astype(jnp.bfloat16)
    q_rope = rotary(query[..., NOPE_DIM:], cos_t[:, None, :], sin_t[:, None, :]).astype(jnp.bfloat16)
    kv_proj = jnp.dot(normed, w_dkv, preferred_element_type=jnp.float32)
    lat_new = rms_norm(kv_proj[:, :KV_LORA], g_kv)
    rope_new = rotary(kv_proj[:, KV_LORA:], cos_t, sin_t).astype(jnp.bfloat16)
    slot_ids = jnp.arange(CACHE_LEN)
    hit_mask = (slot_ids[None, :] == cur_pos[:, None])[:, :, None]
    lat = jnp.where(hit_mask, lat_new[:, None, :], lat)
    rop = jnp.where(hit_mask, rope_new[:, None, :], rop)
    q_lat = jnp.einsum('bhn,chn->bhc', q_nope.astype(jnp.float32), w_uk.astype(jnp.float32)).astype(jnp.bfloat16)
    lat_wide = lat.astype(jnp.float32)
    scores = (jnp.einsum('bhc,btc->bht', q_lat.astype(jnp.float32), lat_wide) + jnp.einsum('bhr,btr->bht', q_rope.astype(jnp.float32), rop.astype(jnp.float32))) * SCORE_SCALE
    visible = slot_ids[None, None, :] <= cur_pos[:, None, None]
    scores = jnp.where(visible, scores, -1e30)
    prob_bf = jax.nn.softmax(scores, axis=-1).astype(jnp.bfloat16)
    o_lat = jnp.einsum('bht,btc->bhc', prob_bf.astype(jnp.float32), lat_wide).astype(jnp.bfloat16)
    heads_out = jnp.einsum('bhc,chv->bhv', o_lat.astype(jnp.float32), w_uv.astype(jnp.float32)).astype(jnp.bfloat16)
    attn_sum = jnp.dot(heads_out.reshape(tokens, NUM_HEADS * V_HEAD), w_out, preferred_element_type=jnp.float32)
    return (hidden.astype(jnp.float32) + attn_sum).astype(jnp.bfloat16), lat, rop


def swiglu(normed, w_gate, w_up, w_down):
    gate_h = jnp.dot(normed, w_gate, preferred_element_type=jnp.float32)
    up_h = jnp.dot(normed, w_up, preferred_element_type=jnp.float32)
    act_bf = (jax.nn.silu(gate_h) * up_h).astype(jnp.bfloat16)
    return jnp.dot(act_bf, w_down, preferred_element_type=jnp.float32)


def routed(normed, expert_ids, router, expert_gate, expert_up, expert_down):
    logits = jnp.dot(normed, router, preferred_element_type=jnp.float32)
    probs_all = jax.nn.softmax(logits, axis=-1)
    route_w = jnp.take_along_axis(probs_all, expert_ids, axis=1)
    combine = jnp.sum(route_w[:, :, None] * (expert_ids[:, :, None] == jnp.arange(EXPERTS)[None, None, :]), axis=1)

    def expert_step(total, packed):
        gate_w, up_w, down_w, weight_col = packed
        return total + weight_col[:, None] * swiglu(normed, gate_w, up_w, down_w), None

    start_sum = jnp.zeros((normed.shape[0], HIDDEN), jnp.float32)
    return lax.scan(expert_step, start_sum, (expert_gate, expert_up, expert_down, combine.T))[0]


def setup_inputs(seed: int = 0, part: int = 0) -> dict:
    base = jax.random.key(seed)
    part_keys = jax.random.split(jax.random.fold_in(base, part), 8)
    weight_keys = jax.random.split(jax.random.fold_in(base, 100003), 18)

    def normal(key, shape):
        return jax.random.normal(key, shape, jnp.float32)

    emb = normal(part_keys[0], (2, TOKENS, HIDDEN)).astype(jnp.bfloat16)
    pos = jax.random.randint(part_keys[1], (TOKENS,), 1, CACHE_LEN - 1, dtype=jnp.int32).at[0].set(CACHE_LEN - 2)
    hot_bias = jax.random.randint(part_keys[2], (EXPERTS,), 0, 3, dtype=jnp.int32) * 64
    raw_score = jax.random.randint(part_keys[3], (2, TOKENS, EXPERTS), 0, 128, dtype=jnp.int32) + hot_bias
    keyed = raw_score * EXPERTS + jnp.arange(EXPERTS, dtype=jnp.int32)
    route_ids = lax.top_k(keyed, TOP_K)[1].astype(jnp.int32)
    lat_cache = (0.5 * normal(part_keys[4], (2, TOKENS, 1, KV_LORA)) + 0.2 * normal(part_keys[5], (2, TOKENS, CACHE_LEN, KV_LORA))).astype(jnp.bfloat16)
    rope_cache = (1.5 * normal(part_keys[6], (2, TOKENS, 1, ROPE_DIM)) + 0.3 * normal(part_keys[7], (2, TOKENS, CACHE_LEN, ROPE_DIM))).astype(jnp.bfloat16)
    q_scale = jnp.where(jnp.arange(QK_DIM) < NOPE_DIM, 1.0, 2.0) * HIDDEN ** -0.5
    return dict(
        emb=emb,
        pos=pos,
        route_ids=route_ids,
        lat_cache=lat_cache,
        rope_cache=rope_cache,
        attn_norm=1.0 + 0.25 * normal(weight_keys[0], (2, HIDDEN)),
        w_q=(normal(weight_keys[1], (2, HIDDEN, NUM_HEADS, QK_DIM)) * q_scale).astype(jnp.bfloat16),
        w_dkv=(normal(weight_keys[2], (2, HIDDEN, KV_LORA + ROPE_DIM)) * HIDDEN ** -0.5).astype(jnp.bfloat16),
        kv_norm=1.0 + 0.25 * normal(weight_keys[3], (2, KV_LORA)),
        w_uk=(normal(weight_keys[4], (2, KV_LORA, NUM_HEADS, NOPE_DIM)) * (LATENT_GAIN * NOPE_DIM ** -0.5)).astype(jnp.bfloat16),
        w_uv=(normal(weight_keys[5], (2, KV_LORA, NUM_HEADS, V_HEAD)) * KV_LORA ** -0.5).astype(jnp.bfloat16),
        w_o=(normal(weight_keys[6], (2, NUM_HEADS * V_HEAD, HIDDEN)) * (NUM_HEADS * V_HEAD) ** -0.5).astype(jnp.bfloat16),
        mlp_norm=1.0 + 0.25 * normal(weight_keys[7], (2, HIDDEN)),
        dense_gate=(normal(weight_keys[8], (HIDDEN, DENSE_FF)) * HIDDEN ** -0.5).astype(jnp.bfloat16),
        dense_up=(normal(weight_keys[9], (HIDDEN, DENSE_FF)) * HIDDEN ** -0.5).astype(jnp.bfloat16),
        dense_down=(normal(weight_keys[10], (DENSE_FF, HIDDEN)) * DENSE_FF ** -0.5).astype(jnp.bfloat16),
        router=(normal(weight_keys[11], (HIDDEN, EXPERTS)) * (1.5 * HIDDEN ** -0.5)).astype(jnp.bfloat16),
        shared_gate=(normal(weight_keys[12], (HIDDEN, SHARED_FF)) * HIDDEN ** -0.5).astype(jnp.bfloat16),
        shared_up=(normal(weight_keys[13], (HIDDEN, SHARED_FF)) * HIDDEN ** -0.5).astype(jnp.bfloat16),
        shared_down=(normal(weight_keys[14], (SHARED_FF, HIDDEN)) * SHARED_FF ** -0.5).astype(jnp.bfloat16),
        expert_gate=(normal(weight_keys[15], (EXPERTS, HIDDEN, EXPERT_FF)) * HIDDEN ** -0.5).astype(jnp.bfloat16),
        expert_up=(normal(weight_keys[16], (EXPERTS, HIDDEN, EXPERT_FF)) * HIDDEN ** -0.5).astype(jnp.bfloat16),
        expert_down=(normal(weight_keys[17], (EXPERTS, EXPERT_FF, HIDDEN)) * (ROUTE_SCALE * EXPERT_FF ** -0.5)).astype(jnp.bfloat16),
    )


def reference(emb, pos, route_ids, lat_cache, rope_cache, attn_norm, w_q, w_dkv, kv_norm, w_uk, w_uv, w_o, mlp_norm, dense_gate, dense_up, dense_down, router, shared_gate, shared_up, shared_down, expert_gate, expert_up, expert_down):
    lat_first, lat_second = lat_cache[0], lat_cache[1]
    rop_first, rop_second = rope_cache[0], rope_cache[1]
    hidden_steps = []
    for step_idx in range(2):
        cur_pos = pos + step_idx
        y_first, lat_first, rop_first = attention(emb[step_idx], cur_pos, lat_first, rop_first, attn_norm[0], w_q[0], w_dkv[0], kv_norm[0], w_uk[0], w_uv[0], w_o[0])
        dense_out = swiglu(rms_norm(y_first, mlp_norm[0]), dense_gate, dense_up, dense_down)
        h_mid = (y_first.astype(jnp.float32) + dense_out).astype(jnp.bfloat16)
        y_second, lat_second, rop_second = attention(h_mid, cur_pos, lat_second, rop_second, attn_norm[1], w_q[1], w_dkv[1], kv_norm[1], w_uk[1], w_uv[1], w_o[1])
        normed = rms_norm(y_second, mlp_norm[1])
        moe_out = swiglu(normed, shared_gate, shared_up, shared_down) + routed(normed, route_ids[step_idx], router, expert_gate, expert_up, expert_down)
        hidden_steps.append((y_second.astype(jnp.float32) + moe_out).astype(jnp.bfloat16))
    return jnp.stack(hidden_steps), jnp.stack([lat_first, lat_second]), jnp.stack([rop_first, rop_second])
```

```python
import functools
import math
import jax
import jax.numpy as jnp
from jax import lax
from jax.experimental import pallas as pl
from jax.experimental.pallas import tpu as pltpu
from jax.sharding import PartitionSpec as P

NORM_EPS = 1e-6
ROPE_THETA = 10000.0
MESH = pl.DeviceIdType.MESH
F32 = jnp.float32
BF16 = jnp.bfloat16
VMEM_ALL = 67043328


def rms_norm(values, gain):
    wide = values.astype(F32)
    mean_sq = jnp.mean(wide * wide, axis=-1, keepdims=True)
    return (wide * lax.rsqrt(mean_sq + NORM_EPS) * gain).astype(BF16)


def rope_tables(position, rope_dim):
    half_dim = rope_dim // 2
    inv_freq = ROPE_THETA ** (-(jnp.arange(half_dim, dtype=F32) * 2.0 / rope_dim))
    angles = position.astype(F32)[:, None] * inv_freq[None, :]
    return jnp.cos(angles), jnp.sin(angles)


def rotary(values, cos_t, sin_t):
    wide = values.astype(F32)
    half_dim = wide.shape[-1] // 2
    first = wide[..., :half_dim]
    second = wide[..., half_dim:]
    return jnp.concatenate([first * cos_t - second * sin_t, second * cos_t + first * sin_t], axis=-1)


def attention(normed, steps, pos, cos_t, sin_t, lat, rop, w_query, w_dkv, g_kv, w_uk, w_uv, w_out):
    rows = normed.shape[0]
    tokens = rows // steps
    heads, nope_dim = w_uk.shape[1], w_uk.shape[2]
    qk_dim = w_query.shape[2]
    lora = g_kv.shape[0]
    cache_len = lat.shape[1]
    query = jnp.einsum('bd,dhk->bhk', normed, w_query, preferred_element_type=F32)
    q_nope = query[..., :nope_dim].astype(BF16)
    q_rope = rotary(query[..., nope_dim:], cos_t[:, None, :], sin_t[:, None, :]).astype(BF16)
    kv_proj = jnp.dot(normed, w_dkv, preferred_element_type=F32)
    lat_new = rms_norm(kv_proj[:, :lora], g_kv).reshape(steps, tokens, -1)
    rope_new = rotary(kv_proj[:, lora:], cos_t, sin_t).astype(BF16).reshape(steps, tokens, -1)
    slot_ids = jnp.arange(cache_len)
    for s in range(steps):
        hit = (slot_ids[None, :] == (pos + s)[:, None])[:, :, None]
        lat = jnp.where(hit, lat_new[s][:, None, :], lat)
        rop = jnp.where(hit, rope_new[s][:, None, :], rop)
    q_lat = jnp.einsum('bhn,chn->bhc', q_nope, w_uk, preferred_element_type=F32).astype(BF16)

    def by_token(v):
        return v.reshape(steps, tokens, heads, -1).transpose(1, 0, 2, 3).reshape(tokens, steps * heads, -1)

    scores = (jnp.einsum('bhc,btc->bht', by_token(q_lat), lat, preferred_element_type=F32)
              + jnp.einsum('bhr,btr->bht', by_token(q_rope), rop, preferred_element_type=F32)) * (1.0 / math.sqrt(qk_dim))
    step_of = jnp.arange(steps * heads) // heads
    visible = slot_ids[None, None, :] <= pos[:, None, None] + step_of[None, :, None]
    scores = jnp.where(visible, scores, -1e30)
    prob = jax.nn.softmax(scores, axis=-1).astype(BF16)
    o_lat = jnp.einsum('bht,btc->bhc', prob, lat, preferred_element_type=F32).astype(BF16)
    o_lat = o_lat.reshape(tokens, steps, heads, -1).transpose(1, 0, 2, 3).reshape(rows, heads, -1)
    heads_out = jnp.einsum('bhc,chv->bhv', o_lat, w_uv, preferred_element_type=F32).astype(BF16)
    part = jnp.dot(heads_out.reshape(rows, -1), w_out, preferred_element_type=F32)
    return part, lat, rop


def swiglu(normed, w_gate, w_up, w_down):
    gate_h = jnp.dot(normed, w_gate, preferred_element_type=F32)
    up_h = jnp.dot(normed, w_up, preferred_element_type=F32)
    act = (jax.nn.silu(gate_h) * up_h).astype(BF16)
    return jnp.dot(act, w_down, preferred_element_type=F32)


def remote(src, dst, send, recv, where):
    return pltpu.make_async_remote_copy(src_ref=src, dst_ref=dst, send_sem=send, recv_sem=recv,
                                        device_id=where, device_id_type=MESH)


def turn(me, d, n):
    return lax.rem(me + d, n)


def reduce_kernel(n_tp, n_ep, with_ids, *refs):
    if with_ids:
        (part, resid, gain, ids, own_out, norm_out, ids_out,
         recv, gath, ids_all, s1, r1, s2, r2, s3, r3) = refs
    else:
        part, resid, gain, own_out, norm_out, recv, gath, s1, r1, s2, r2 = refs
    me = lax.axis_index("tp")
    rows = part.shape[0] // n_tp
    barrier = pltpu.get_barrier_semaphore()
    for d in range(1, n_tp):
        pl.semaphore_signal(barrier, inc=1, device_id={"tp": turn(me, d, n_tp)}, device_id_type=MESH)
    if with_ids:
        ep = lax.axis_index("ep")
        for d in range(1, n_ep):
            pl.semaphore_signal(barrier, inc=1, device_id={"ep": turn(ep, d, n_ep)}, device_id_type=MESH)
    pl.semaphore_wait(barrier, n_tp - 1 + (n_ep - 1 if with_ids else 0))
    sends = []
    for d in range(1, n_tp):
        peer = turn(me, d, n_tp)
        cp = remote(part.at[pl.ds(peer * rows, rows)], recv.at[d - 1], s1.at[d - 1], r1.at[d - 1], {"tp": peer})
        cp.start()
        sends.append(cp)
    id_sends = []
    if with_ids:
        for d in range(1, n_ep):
            cp = remote(ids, ids_all.at[ep], s3.at[d - 1], r3.at[d - 1], {"ep": turn(ep, d, n_ep)})
            cp.start()
            id_sends.append(cp)
        ids_out[ep] = ids[...]
    own_rows = pl.ds(me * rows, rows)
    base = resid[own_rows, :] if resid.shape[0] != rows else resid[...]
    total = part[own_rows, :]
    for d in range(1, n_tp):
        sends[d - 1].wait_recv()
        total = total + recv[d - 1]
    y = (base.astype(F32) + total).astype(BF16)
    own_out[...] = y
    normed = rms_norm(y, gain[...])
    gath[me] = normed
    gathers = []
    for d in range(1, n_tp):
        cp = remote(gath.at[me], gath.at[me], s2.at[d - 1], r2.at[d - 1], {"tp": turn(me, d, n_tp)})
        cp.start()
        gathers.append(cp)
    norm_out[own_rows, :] = normed
    for d in range(1, n_tp):
        gathers[d - 1].wait_recv()
        src = turn(me, n_tp - d, n_tp)
        norm_out[pl.ds(src * rows, rows), :] = gath[src]
    if with_ids:
        for d in range(1, n_ep):
            id_sends[d - 1].wait_recv()
            src = turn(ep, n_ep - d, n_ep)
            ids_out[src] = ids_all[src]
    for cp in sends + gathers + id_sends:
        cp.wait_send()


def reduce_norm(n_tp, n_ep, part, resid, gain, ids=None):
    rows, hidden = part.shape
    own = rows // n_tp
    out_shape = [jax.ShapeDtypeStruct((own, hidden), BF16), jax.ShapeDtypeStruct((rows, hidden), BF16)]
    scratch = [pltpu.VMEM((n_tp - 1, own, hidden), F32), pltpu.VMEM((n_tp, own, hidden), BF16)]
    sems = [pltpu.SemaphoreType.DMA((n_tp - 1,))] * 4
    args = [part, resid, gain[None, :]]
    if ids is not None:
        args.append(ids)
        out_shape.append(jax.ShapeDtypeStruct((n_ep,) + ids.shape, ids.dtype))
        scratch.append(pltpu.VMEM((n_ep,) + ids.shape, ids.dtype))
        sems += [pltpu.SemaphoreType.DMA((n_ep - 1,))] * 2
    vm = pl.BlockSpec(memory_space=pltpu.VMEM)
    return pl.pallas_call(
        functools.partial(reduce_kernel, n_tp, n_ep, ids is not None),
        out_shape=out_shape,
        in_specs=[vm] * len(args),
        out_specs=[vm] * len(out_shape),
        scratch_shapes=scratch + sems,
        compiler_params=pltpu.CompilerParams(collective_id=0 if ids is None else 1, has_side_effects=True),
        name="reduce_norm_ids" if ids is not None else "reduce_norm",
    )(*args)


def moe_kernel(n_tp, n_ep, part, resid, gain, router, ids, sg, su, sd, eg, eu, ed, out,
               wg, wu, wd, vg, vu, vd, xs, y_own, recv, comb, acc, drecv, xrecv, shbuf, yrecv, obuf,
               wsem, vsem, s1, r1, sx, rx, sy, ry, sd2, rd2, sa, ra, sb, rb, sc, rc, so, ro):
    me = lax.axis_index("tp")
    ep = lax.axis_index("ep")
    xi, core = ep // 2, lax.rem(ep, 2)
    n_x = n_ep // 2
    partner = ep + 1 - 2 * core
    rows = part.shape[0] // n_tp
    hidden = part.shape[1]
    block = part.shape[0]
    n_exp = wg.shape[0]

    loads = []
    for i, (src, dst) in enumerate(((sg, vg), (su, vu), (sd, vd))):
        cp = pltpu.make_async_copy(src, dst, vsem.at[i])
        cp.start()
        loads.append(cp)
    for e in range(n_exp):
        for i, (src, dst) in enumerate(((eg, wg), (eu, wu), (ed, wd))):
            pltpu.make_async_copy(src.at[e], dst.at[e], wsem.at[i, e]).start()

    barrier = pltpu.get_barrier_semaphore()
    for d in range(1, n_tp):
        pl.semaphore_signal(barrier, inc=1, device_id={"tp": turn(me, d, n_tp)}, device_id_type=MESH)
    for d in range(1, n_x):
        pl.semaphore_signal(barrier, inc=1, device_id={"ep": turn(ep, 2 * d, n_ep)}, device_id_type=MESH)
    pl.semaphore_signal(barrier, inc=1, device_id={"ep": partner}, device_id_type=MESH)
    pl.semaphore_wait(barrier, n_tp - 1 + n_x - 1 + 1)

    pend = []
    cps = []
    for d in range(1, n_tp):
        peer = turn(me, d, n_tp)
        cp = remote(part.at[pl.ds(peer * rows, rows)], recv.at[d - 1], s1.at[d - 1], r1.at[d - 1], {"tp": peer})
        cp.start()
        cps.append(cp)
    total = part[pl.ds(me * rows, rows), :]
    for d in range(1, n_tp):
        cps[d - 1].wait_recv()
        total = total + recv[d - 1]
    pend += cps
    y = (resid[...].astype(F32) + total).astype(BF16)
    y_own[...] = y
    xs[ep, me] = rms_norm(y, gain[...])

    xcp, ycp = [], {}
    for d in range(1, n_x):
        cp = remote(xs.at[ep, me], xs.at[ep, me], sx.at[d - 1], rx.at[d - 1], {"ep": turn(ep, 2 * d, n_ep)})
        cp.start()
        xcp.append(cp)
    for k in range(n_x):
        src_ep = turn(ep, n_ep - 2 * k, n_ep)
        if k:
            xcp[k - 1].wait_recv()
        for d in range(1, n_tp):
            cp = remote(xs.at[src_ep, me], xs.at[src_ep, me], sy.at[k, d - 1], ry.at[k, d - 1], {"tp": turn(me, d, n_tp)})
            cp.start()
            ycp[k, d] = cp
    pcp = []
    for k in range(n_x):
        src_ep = turn(ep, n_ep - 2 * k, n_ep)
        for d in range(1, n_tp):
            ycp[k, d].wait_recv()
        cp = remote(xs.at[src_ep], xs.at[src_ep], sd2.at[k], rd2.at[k], {"ep": partner})
        cp.start()
        pcp.append(cp)
    pend += xcp + list(ycp.values()) + pcp

    for cp in loads:
        cp.wait()
    own = xs[ep].reshape(block, hidden)
    sact = (jax.nn.silu(jnp.dot(own, vg[...], preferred_element_type=F32))
            * jnp.dot(own, vu[...], preferred_element_type=F32)).astype(BF16)
    shbuf[...] = jnp.dot(sact, vd[...], preferred_element_type=F32)
    for cp in pcp:
        cp.wait_recv()

    for k in range(n_x):
        xk = xs[2 * k:2 * k + 2].reshape(2 * block, hidden)
        logits = jnp.dot(xk, router[...], preferred_element_type=F32)
        top = jnp.max(logits, axis=-1, keepdims=True)
        ex = jnp.exp(logits - top)
        prob = ex / jnp.sum(ex, axis=-1, keepdims=True)
        lane = lax.broadcasted_iota(jnp.int32, prob.shape, 1)
        picks = ids[2 * k:2 * k + 2].reshape(2 * block, ids.shape[-1])
        chosen = lane == picks[:, 0:1]
        for j in range(1, TOP_K[0]):
            chosen = chosen | (lane == picks[:, j:j + 1])
        comb[k] = jnp.where(chosen, prob, 0.0)

    n_col = 4
    width = hidden // n_col

    def experts(slot, xb, first, lo, hi):
        def body(e, _):
            if first:
                for i, (src, dst) in enumerate(((eg, wg), (eu, wu), (ed, wd))):
                    pltpu.make_async_copy(src.at[e], dst.at[e], wsem.at[i, e]).wait()
            xk = xs[pl.ds(2 * xb, 2)].reshape(2 * block, hidden)
            gate = jnp.dot(xk, wg[e], preferred_element_type=F32)
            up = jnp.dot(xk, wu[e], preferred_element_type=F32)
            act = (jax.nn.silu(gate) * up).astype(BF16)
            cw = comb[xb]
            lane = lax.broadcasted_iota(jnp.int32, cw.shape, 1)
            col = jnp.sum(jnp.where(lane == ep * n_exp + e, cw, 0.0), axis=-1, keepdims=True)
            for q in range(n_col):
                cs = slice(q * width, (q + 1) * width)
                acc[slot, :, cs] += col * jnp.dot(act, wd[e, :, cs], preferred_element_type=F32)
            return 0
        lax.fori_loop(lo, hi, body, 0)

    order = [2, 1, 3, 0] if n_x == 4 else list(range(1, n_x)) + [0]
    dcp, acp = {}, {}
    mine = pl.ds(core * block, block)
    other = pl.ds((1 - core) * block, block)

    def settle(b):
        dcp[b].wait_recv()
        drecv[b] = drecv[b] + acc[b % 2, mine, :]
        d = order[b]
        if d:
            cp = remote(drecv.at[b], xrecv.at[d - 1], sa.at[d - 1], ra.at[d - 1], {"ep": turn(ep, 2 * d, n_ep)})
            cp.start()
            acp[d] = cp
        dcp[b].wait_send()

    half = n_exp // 2
    for b, d in enumerate(order):
        slot = b % 2
        xb = lax.rem(xi + d, n_x)
        acc[slot] = jnp.zeros(acc.shape[1:], F32)
        experts(slot, xb, b == 0, 0, half)
        if b:
            settle(b - 1)
        experts(slot, xb, b == 0, half, n_exp)
        cp = remote(acc.at[slot, other], drecv.at[b], sb.at[b], rb.at[b], {"ep": partner})
        cp.start()
        dcp[b] = cp
    last = n_x - 1
    settle(last)
    drecv[last] = drecv[last] + shbuf[...]
    for d in range(1, n_x):
        acp[d].wait_recv()
        drecv[last] = drecv[last] + xrecv[d - 1]
    pend += list(acp.values())
    ccp = []
    for d in range(1, n_tp):
        peer = turn(me, d, n_tp)
        cp = remote(drecv.at[last, pl.ds(peer * rows, rows)], yrecv.at[d - 1], sc.at[d - 1], rc.at[d - 1], {"tp": peer})
        cp.start()
        ccp.append(cp)
    total = drecv[last, pl.ds(me * rows, rows), :]
    for d in range(1, n_tp):
        ccp[d - 1].wait_recv()
        total = total + yrecv[d - 1]
    fin = (y_own[...].astype(F32) + total).astype(BF16)
    obuf[me] = fin
    ocp = []
    for d in range(1, n_tp):
        cp = remote(obuf.at[me], obuf.at[me], so.at[d - 1], ro.at[d - 1], {"tp": turn(me, d, n_tp)})
        cp.start()
        ocp.append(cp)
    out[pl.ds(me * rows, rows), :] = fin
    for d in range(1, n_tp):
        ocp[d - 1].wait_recv()
        src = turn(me, n_tp - d, n_tp)
        out[pl.ds(src * rows, rows), :] = obuf[src]
    for cp in pend + ccp + ocp:
        cp.wait_send()


TOP_K = [6]


def moe(n_tp, n_ep, part, resid, gain, router, ids, sg, su, sd, eg, eu, ed):
    rows, hidden = part.shape
    own = rows // n_tp
    n_x = n_ep // 2
    dma = pltpu.SemaphoreType.DMA
    n_exp = eg.shape[0]
    vm = pl.BlockSpec(memory_space=pltpu.VMEM)
    hbm = pl.BlockSpec(memory_space=pl.ANY)
    scratch = [
        pltpu.VMEM(eg.shape, BF16), pltpu.VMEM(eu.shape, BF16), pltpu.VMEM(ed.shape, BF16),
        pltpu.VMEM(sg.shape, BF16), pltpu.VMEM(su.shape, BF16), pltpu.VMEM(sd.shape, BF16),
        pltpu.VMEM((n_ep, n_tp, own, hidden), BF16),
        pltpu.VMEM((own, hidden), BF16),
        pltpu.VMEM((n_tp - 1, own, hidden), F32),
        pltpu.VMEM((n_x, 2 * rows, router.shape[1]), F32),
        pltpu.VMEM((2, 2 * rows, hidden), F32),
        pltpu.VMEM((n_x, rows, hidden), F32),
        pltpu.VMEM((n_x - 1, rows, hidden), F32),
        pltpu.VMEM((rows, hidden), F32),
        pltpu.VMEM((n_tp - 1, own, hidden), F32),
        pltpu.VMEM((n_tp, own, hidden), BF16),
        dma((3, n_exp)), dma((3,)),
        dma((n_tp - 1,)), dma((n_tp - 1,)),
        dma((n_x - 1,)), dma((n_x - 1,)),
        dma((n_x, n_tp - 1)), dma((n_x, n_tp - 1)),
        dma((n_x,)), dma((n_x,)),
        dma((n_x - 1,)), dma((n_x - 1,)),
        dma((n_x,)), dma((n_x,)),
        dma((n_tp - 1,)), dma((n_tp - 1,)),
        dma((n_tp - 1,)), dma((n_tp - 1,)),
    ]
    return pl.pallas_call(
        functools.partial(moe_kernel, n_tp, n_ep),
        out_shape=jax.ShapeDtypeStruct((rows, hidden), BF16),
        in_specs=[vm] * 5 + [hbm] * 6,
        out_specs=vm,
        scratch_shapes=scratch,
        compiler_params=pltpu.CompilerParams(collective_id=2, has_side_effects=True, vmem_limit_bytes=VMEM_ALL),
        name="moe",
    )(part, resid, gain[None, :], router, ids, sg, su, sd, eg, eu, ed)


def solution(mesh):
    tok_axes = ('dp', 'ep')
    n_tp, n_ep = mesh.shape['tp'], mesh.shape['ep']

    def device_fn(emb, pos, route_ids, lat_cache, rope_cache, attn_norm, w_q, w_dkv, kv_norm, w_uk, w_uv, w_o, mlp_norm, dense_gate, dense_up, dense_down, router, shared_gate, shared_up, shared_down, expert_gate, expert_up, expert_down):
        steps, tokens, hidden = emb.shape
        rows = steps * tokens
        TOP_K[0] = route_ids.shape[-1]
        emb_rows = emb.reshape(rows, hidden)
        ids = jnp.pad(route_ids.reshape(rows, -1), ((0, 0), (0, 128 - route_ids.shape[-1])), constant_values=-1)
        all_pos = jnp.concatenate([pos + s for s in range(steps)])
        cos_t, sin_t = rope_tables(all_pos, rope_cache.shape[-1])

        def attend(layer, normed):
            return attention(normed, steps, pos, cos_t, sin_t, lat_cache[layer], rope_cache[layer], w_q[layer], w_dkv[layer], kv_norm[layer], w_uk[layer], w_uv[layer], w_o[layer])

        part, lat0, rop0 = attend(0, rms_norm(emb_rows, attn_norm[0]))
        y_own, normed, ids_all = reduce_norm(n_tp, n_ep, part, emb_rows, mlp_norm[0], ids)
        part = swiglu(normed, dense_gate, dense_up, dense_down)
        h_own, normed = reduce_norm(n_tp, n_ep, part, y_own, attn_norm[1])
        part, lat1, rop1 = attend(1, normed)
        out = moe(n_tp, n_ep, part, h_own, mlp_norm[1], router, ids_all, shared_gate, shared_up, shared_down, expert_gate, expert_up, expert_down)
        return out.reshape(steps, tokens, hidden), jnp.stack([lat0, lat1]), jnp.stack([rop0, rop1])

    in_specs = (P(None, tok_axes, None), P(tok_axes), P(None, tok_axes, None), P(None, tok_axes, None, None), P(None, tok_axes, None, None), P(), P(None, None, 'tp', None), P(), P(), P(None, None, 'tp', None), P(None, None, 'tp', None), P(None, 'tp', None), P(), P(None, 'tp'), P(None, 'tp'), P('tp', None), P(), P(None, 'tp'), P(None, 'tp'), P('tp', None), P('ep', None, 'tp'), P('ep', None, 'tp'), P('ep', 'tp', None))
    out_specs = (P(None, tok_axes, None), P(None, tok_axes, None, None), P(None, tok_axes, None, None))
    return jax.shard_map(device_fn, mesh=mesh, in_specs=in_specs, out_specs=out_specs, check_vma=False)
```

```python
import functools
import math
import jax
import jax.numpy as jnp
import numpy as np
from jax import lax
from jax.experimental import pallas as pl
from jax.experimental.pallas import tpu as pltpu
from jax.sharding import PartitionSpec as P

NORM_EPS = 1e-6
ROPE_THETA = 10000.0
MESH = pl.DeviceIdType.MESH
F32 = jnp.float32
BF16 = jnp.bfloat16
VMEM_ALL = 67043328


def rms_norm(values, gain):
    wide = values.astype(F32)
    mean_sq = jnp.mean(wide * wide, axis=-1, keepdims=True)
    return (wide * lax.rsqrt(mean_sq + NORM_EPS) * gain).astype(BF16)


def nt(a, b):
    return lax.dot_general(a, b, (((1,), (1,)), ((), ())), preferred_element_type=F32)


def nn(a, b):
    return jnp.dot(a, b, preferred_element_type=F32)


def silu_mul(gate, up):
    return (jax.nn.silu(gate) * up).astype(BF16)


def attn_kernel(layer, steps, group, *refs):
    n_in = 13 if layer == 0 else 15
    (x, gain, pos, pos_row, freq, g_kv, wq, wdkv, wuk, wuv, wo, lat, rop) = refs[:13]
    part, lat_out, rop_out = refs[n_in:n_in + 3]
    (wqb, wdkvb, wukb, wuvb, wob, latb, ropb, qls, qrs, latn, ropn, outs, wide,
     wsem, csem, osem) = refs[n_in + 3:]
    lora = g_kv.shape[1]
    tok = latb.shape[0]
    cache = latb.shape[1]
    rope = ropb.shape[1]
    half = rope // 2
    heads = outs.shape[1] // (steps * tok)
    qk = wqb.shape[0] // heads
    nope = qk - rope
    scale = 1.0 / math.sqrt(qk)
    per = steps * heads
    n_group = tok // group

    loads = []
    for i, (src, dst) in enumerate(((wq, wqb), (wdkv, wdkvb), (wuk, wukb), (wuv, wuvb), (wo, wob))):
        loads.append(pltpu.make_async_copy(src.at[layer], dst, wsem.at[i]))

    def cache_in(g):
        t = pl.ds(g * group, group)
        return (pltpu.make_async_copy(lat.at[layer, t], latb.at[t], csem.at[0, g]),
                pltpu.make_async_copy(rop.at[layer, t], ropb.at[t], csem.at[1, g]))

    def cache_out(g):
        t = pl.ds(g * group, group)
        return (pltpu.make_async_copy(latb.at[t], lat_out.at[layer, t], osem.at[0, g]),
                pltpu.make_async_copy(ropb.at[t], rop_out.at[layer, t], osem.at[1, g]))

    for cp in loads[:3]:
        cp.start()

    places = jnp.concatenate([pos_row[...] + s for s in range(steps)], axis=1).astype(F32)
    angle = freq[...] * places
    cos_t, sin_t = jnp.cos(angle), jnp.sin(angle)
    first = lax.broadcasted_iota(jnp.int32, angle.shape, 0) < half
    cosf, sinf = jnp.transpose(cos_t), jnp.transpose(jnp.where(first, -sin_t, sin_t))
    cost, sint = cos_t[:half], sin_t[:half]

    normed = rms_norm(x[...], gain[layer:layer + 1, :]) if layer == 0 else x[...]
    loads[0].wait()
    for g in range(n_group):
        for cp in cache_in(g):
            cp.start()
    for cp in loads[3:]:
        cp.start()
    query = nt(normed, wqb[...])
    loads[1].wait()
    kv = nt(normed, wdkvb[:lora, :])
    latn[...] = rms_norm(kv, g_kv[layer:layer + 1, :]).astype(F32)
    key = nt(wdkvb[lora:, :], normed)
    k1, k2 = key[:half], key[half:]
    ropn[...] = jnp.concatenate([k1 * cost - k2 * sint, k2 * cost + k1 * sint], axis=0).astype(BF16).astype(F32)
    loads[2].wait()
    wide[...] = wukb[...].astype(F32)
    for h in range(heads):
        base = h * qk
        qn = query[:, base:base + nope].astype(BF16)
        pe = query[:, base + nope:base + qk]
        swapped = jnp.concatenate([pe[:, half:], pe[:, :half]], axis=1)
        turned = pe * cosf + swapped * sinf
        ql = nt(qn, wide[pl.ds(h, lora, stride=heads), :].astype(BF16))
        for s in range(steps):
            at = slice((s * heads + h) * tok, (s * heads + h + 1) * tok)
            qrs[at, :rope] = turned[s * tok:(s + 1) * tok]
            for c in range(lora // 128):
                qls[c, at, :] = ql[s * tok:(s + 1) * tok, c * 128:(c + 1) * 128]

    row16 = lax.broadcasted_iota(jnp.int32, (16, lora), 0)
    lane_c = lax.broadcasted_iota(jnp.int32, (rope, cache), 1)
    lane_r = lax.broadcasted_iota(jnp.int32, (rope, steps * tok), 1)
    lane_s = lax.broadcasted_iota(jnp.int32, (per, cache), 1)
    step_s = lax.broadcasted_iota(jnp.int32, (per, cache), 0) // heads

    def run_group(g, _):
        for cp in cache_in(g):
            cp.wait()
        for j in range(group):
            b = g * group + j
            p = pos[b]
            rb = ropb[b].astype(F32)
            for s in range(steps):
                slot = p + s
                start = pl.multiple_of((slot // 16) * 16, 16)
                old = latb[b, pl.ds(start, 16), :].astype(F32)
                new = latn[pl.ds(s * tok + b, 1), :]
                latb[b, pl.ds(start, 16), :] = jnp.where(row16 == slot - start, new, old).astype(BF16)
                col = jnp.sum(jnp.where(lane_r == s * tok + b, ropn[...], 0.0), axis=1, keepdims=True)
                rb = jnp.where(lane_c == slot, col, rb)
            ropb[b] = rb.astype(BF16)
        for cp in cache_out(g):
            cp.start()
        probs = []
        for j in range(group):
            b = g * group + j
            mine = pl.ds(b, per, stride=tok)
            ql = jnp.concatenate([qls[c, mine, :] for c in range(lora // 128)], axis=1).astype(BF16)
            qr = qrs[mine, :][:, :rope].astype(BF16)
            sc = (nt(ql, latb[b]) + nn(qr, ropb[b])) * scale
            sc = jnp.where(lane_s <= pos[b] + step_s, sc, -1e30)
            ex = jnp.exp(sc - jnp.max(sc, axis=-1, keepdims=True))
            probs.append((ex / jnp.sum(ex, axis=-1, keepdims=True)).astype(BF16))
        for j in range(group):
            b = g * group + j
            val = nn(probs[j], latb[b])
            for c in range(lora // 128):
                outs[c, pl.ds(b, per, stride=tok), :] = val[:, c * 128:(c + 1) * 128]
        return 0

    lax.fori_loop(0, n_group, run_group, 0)
    loads[3].wait()
    wide[...] = wuvb[...].astype(F32)
    vals = []
    for h in range(heads):
        ol = jnp.concatenate([
            jnp.concatenate([outs[c, (s * heads + h) * tok:(s * heads + h + 1) * tok, :] for s in range(steps)], axis=0)
            for c in range(lora // 128)], axis=1).astype(BF16)
        vals.append(nn(ol, wide[pl.ds(h, lora, stride=heads), :].astype(BF16)).astype(BF16))
    loads[4].wait()
    part[...] = nn(jnp.concatenate(vals, axis=1), wob[...])
    for g in range(n_group):
        for cp in cache_out(g):
            cp.wait()


def attention(layer, steps, x, gain, pos, freq, g_kv, wq, wdkv, wuk, wuv, wo, lat, rop, outs):
    rows = x.shape[0]
    tok, cache, lora = lat.shape[1:]
    rope = rop.shape[2]
    hidden = wo.shape[2]
    heads = wq.shape[1]
    qk = wq.shape[2]
    group = 8
    vm = pl.BlockSpec(memory_space=pltpu.VMEM)
    hbm = pl.BlockSpec(memory_space=pl.ANY)
    sm = pl.BlockSpec(memory_space=pltpu.SMEM)
    wq2 = wq.reshape(wq.shape[0], heads * qk, -1)
    args = [x, gain, pos, pos[None, :], freq, g_kv, wq2, wdkv, wuk, wuv, wo, lat, rop]
    specs = [vm, vm, sm] + [vm] * 3 + [hbm] * 7
    alias = {}
    if outs is not None:
        args += list(outs)
        specs += [hbm, hbm]
        alias = {13: 1, 14: 2}
    dma = pltpu.SemaphoreType.DMA
    return pl.pallas_call(
        functools.partial(attn_kernel, layer, steps, group),
        out_shape=[jax.ShapeDtypeStruct((rows, hidden), F32),
                   jax.ShapeDtypeStruct(lat.shape, BF16), jax.ShapeDtypeStruct(rop.shape, BF16)],
        in_specs=specs,
        out_specs=[vm, hbm, hbm],
        input_output_aliases=alias,
        scratch_shapes=[
            pltpu.VMEM(wq2.shape[1:], BF16), pltpu.VMEM(wdkv.shape[1:], BF16), pltpu.VMEM(wuk.shape[1:], BF16),
            pltpu.VMEM(wuv.shape[1:], BF16), pltpu.VMEM(wo.shape[1:], BF16),
            pltpu.VMEM((tok, cache, lora), BF16), pltpu.VMEM((tok, rope, cache), BF16),
            pltpu.VMEM((lora // 128, rows * heads, 128), F32), pltpu.VMEM((rows * heads, 128), F32),
            pltpu.VMEM((rows, lora), F32), pltpu.VMEM((rope, rows), F32), pltpu.VMEM((lora // 128, rows * heads, 128), F32),
            pltpu.VMEM(wuk.shape[1:], F32),
            dma((5,)), dma((2, tok // group)), dma((2, tok // group)),
        ],
        compiler_params=pltpu.CompilerParams(vmem_limit_bytes=VMEM_ALL),
        name="attn%d" % layer,
    )(*args)


def remote(src, dst, send, recv, where):
    return pltpu.make_async_remote_copy(src_ref=src, dst_ref=dst, send_sem=send, recv_sem=recv,
                                        device_id=where, device_id_type=MESH)


def turn(me, d, n):
    return lax.rem(me + d, n)


def fetch(refs, sem):
    half = len(refs) // 2
    cps = [pltpu.make_async_copy(src, dst, sem.at[i]) for i, (src, dst) in enumerate(zip(refs[:half], refs[half:]))]
    for cp in cps:
        cp.start()
    return cps, refs[half:]


def rows_reduce(part, bufs, sems, me, n_tp, rows):
    relay, fin = bufs
    hidden = part.shape[1]
    lo, hi = pl.ds(0, hidden // 2), pl.ds(hidden // 2, hidden // 2)
    up, far, down = turn(me, 1, n_tp), turn(me, 2, n_tp), turn(me, n_tp - 1, n_tp)

    def at(owner):
        return pl.ds(owner * rows, rows)

    def send(src, dst, i, peer):
        cp = remote(src, dst, sems[0].at[i], sems[1].at[i], {"tp": peer})
        cp.start()
        return cp

    cps = [send(part.at[at(far), lo], relay.at[0], 0, up), send(part.at[at(far), hi], relay.at[1], 1, down),
           send(part.at[at(up), hi], fin.at[0, :, hi], 2, up), send(part.at[at(down), lo], fin.at[1, :, lo], 3, down)]
    cps[0].wait_recv()
    relay[0] = relay[0] + part[at(up), lo]
    cps.append(send(relay.at[0], fin.at[0, :, lo], 4, up))
    cps[1].wait_recv()
    relay[1] = relay[1] + part[at(down), hi]
    cps.append(send(relay.at[1], fin.at[1, :, hi], 5, down))
    for cp in cps[2:]:
        cp.wait_recv()
    return part[at(me), :] + (fin[0] + fin[1]), cps


def reduce_scratch(own, hidden):
    return [pltpu.VMEM((2, own, hidden // 2), F32), pltpu.VMEM((2, own, hidden), F32)]


def rows_gather(buf, s, r, me, n_tp):
    cps = []
    for d in range(1, n_tp):
        cp = remote(buf.at[me], buf.at[me], s.at[d - 1], r.at[d - 1], {"tp": turn(me, d, n_tp)})
        cp.start()
        cps.append(cp)
    return cps


def mid_kernel(n_tp, n_ep, step, part_in, resid_in, gain0_in, gain1_in, ids_in, wg, wu, wd,
               own_out, norm_out, ids_out, part, resid, gain0, gain1, ids, in_sem,
               wgb, wub, wdb, relay0, recv0, relay1, recv1, gath0, gath1, acc, ids_own, ids_all,
               wsem, s1, r1, s2, r2, s3, r3, s4, r4, s5, r5):
    me = lax.axis_index("tp")
    ep = lax.axis_index("ep")
    total_rows, hidden = part.shape
    rows = total_rows // n_tp
    first, _ = fetch((part_in, resid_in, gain0_in, gain1_in, ids_in, part, resid, gain0, gain1, ids), in_sem)
    barrier = pltpu.get_barrier_semaphore()
    for d in range(1, n_tp):
        pl.semaphore_signal(barrier, inc=1, device_id={"tp": turn(me, d, n_tp)}, device_id_type=MESH)
    for d in range(1, n_ep):
        pl.semaphore_signal(barrier, inc=1, device_id={"ep": turn(ep, d, n_ep)}, device_id_type=MESH)
    pl.semaphore_wait(barrier, n_tp - 1 + n_ep - 1)
    for cp in first:
        cp.wait()
    loads = []
    for i, (src, dst) in enumerate(((wg, wgb), (wu, wub), (wd, wdb))):
        cp = pltpu.make_async_copy(src, dst, wsem.at[i])
        cp.start()
        loads.append(cp)

    id_cps = []
    picks = jnp.concatenate([ids[:, i, :] for i in range(ids.shape[1])], axis=1).astype(F32)
    picks = jnp.concatenate([picks, jnp.zeros((8 - picks.shape[0], picks.shape[1]), F32)], axis=0)
    ids_own[...] = jnp.zeros(ids_own.shape, jnp.int32)
    ids_own[:, 0:8] = jnp.transpose(picks).astype(jnp.int32)
    for d in range(1, n_ep):
        cp = remote(ids_own, ids_all.at[ep], s5.at[d - 1], r5.at[d - 1], {"ep": turn(ep, d, n_ep)})
        cp.start()
        id_cps.append(cp)
    ids_out[ep] = ids_own[...]
    own = pl.ds(me * rows, rows)
    total, red0 = rows_reduce(part, (relay0, recv0), (s1, r1), me, n_tp, rows)
    y = (resid[own, :].astype(F32) + total).astype(BF16)
    gath0[me] = rms_norm(y, gain0[0:1, :])
    gat0 = rows_gather(gath0, s2, r2, me, n_tp)
    for cp in loads:
        cp.wait()
    for cp in gat0:
        cp.wait_recv()

    width = wgb.shape[0]

    def chunk(start, size, first):
        x = gath0[...].reshape(total_rows, hidden)
        act = silu_mul(nt(x, wgb[pl.ds(start, size), :]), nt(x, wub[pl.ds(start, size), :]))
        down = nn(act, wdb[pl.ds(start, size), :])
        acc[...] = down if first else acc[...] + down

    whole = width // step
    chunk(0, step, True)

    def body(i, _):
        chunk(pl.multiple_of(i * step, step), step, False)
        return 0

    lax.fori_loop(1, whole, body, 0)
    if width % step:
        chunk(whole * step, width % step, False)

    total, red1 = rows_reduce(acc, (relay1, recv1), (s3, r3), me, n_tp, rows)
    h = (y.astype(F32) + total).astype(BF16)
    own_out[...] = h
    normed = rms_norm(h, gain1[1:2, :])
    gath1[me] = normed
    gat1 = rows_gather(gath1, s4, r4, me, n_tp)
    norm_out[own, :] = normed
    for d in range(1, n_ep):
        id_cps[d - 1].wait_recv()
        src = turn(ep, n_ep - d, n_ep)
        ids_out[src] = ids_all[src]
    for d in range(1, n_tp):
        gat1[d - 1].wait_recv()
        src = turn(me, n_tp - d, n_tp)
        norm_out[pl.ds(src * rows, rows), :] = gath1[src]
    for cp in red0 + gat0 + red1 + gat1 + id_cps:
        cp.wait_send()


def mid(n_tp, n_ep, part, resid, gain0, gain1, ids, wg, wu, wd):
    rows, hidden = part.shape
    first = (part, resid, gain0, gain1, ids)
    own = rows // n_tp
    dma = pltpu.SemaphoreType.DMA
    vm = pl.BlockSpec(memory_space=pltpu.VMEM)
    hbm = pl.BlockSpec(memory_space=pl.ANY)
    return pl.pallas_call(
        functools.partial(mid_kernel, n_tp, n_ep, 512),
        out_shape=[jax.ShapeDtypeStruct((own, hidden), BF16), jax.ShapeDtypeStruct((rows, hidden), BF16),
                   jax.ShapeDtypeStruct((n_ep, rows, 128), ids.dtype)],
        in_specs=[hbm] * 8,
        out_specs=[vm] * 3,
        scratch_shapes=[
            *[pltpu.VMEM(v.shape, v.dtype) for v in first], dma((len(first),)),
            pltpu.VMEM(wg.shape, BF16), pltpu.VMEM(wu.shape, BF16), pltpu.VMEM(wd.shape, BF16),
            *reduce_scratch(own, hidden), *reduce_scratch(own, hidden),
            pltpu.VMEM((n_tp, own, hidden), BF16), pltpu.VMEM((n_tp, own, hidden), BF16),
            pltpu.VMEM((rows, hidden), F32), pltpu.VMEM((rows, 128), ids.dtype), pltpu.VMEM((n_ep, rows, 128), ids.dtype),
            dma((3,))] + [dma((6,)), dma((6,)), dma((n_tp - 1,)), dma((n_tp - 1,))] * 2 + [dma((n_ep - 1,))] * 2,
        compiler_params=pltpu.CompilerParams(collective_id=0, has_side_effects=True, vmem_limit_bytes=VMEM_ALL),
        name="mid",
    )(*first, wg, wu, wd)


def moe_kernel(n_tp, n_ep, top_k, part_in, resid_in, gain_in, router_in, ids_in, sg, su, sd, eg, eu, ed, out,
               part, resid, gain, router, ids, in_sem,
               wg, wu, wd, vg, vu, vd, xs, y_own, relay0, recv0, comb, acc, drecv, xrelay, xrecv, shbuf, xpair, acts,
               relay1, recv1, obuf,
               wsem, vsem, s1, r1, sx, rx, sy, ry, sz, rz, sd2, rd2, sa, ra, sb, rb, sc, rc, so, ro):
    me = lax.axis_index("tp")
    ep = lax.axis_index("ep")
    xi, core = ep // 2, lax.rem(ep, 2)
    n_x = n_ep // 2
    partner = ep + 1 - 2 * core
    rows = part.shape[0] // n_tp
    hidden = part.shape[1]
    block = part.shape[0]
    n_exp = wg.shape[0]
    lo, hi = pl.ds(0, hidden // 2), pl.ds(hidden // 2, hidden // 2)
    up, down = turn(me, 1, n_tp), turn(me, n_tp - 1, n_tp)

    start, _ = fetch((part_in, resid_in, gain_in, router_in, ids_in, part, resid, gain, router, ids), in_sem)
    barrier = pltpu.get_barrier_semaphore()
    for d in range(1, n_tp):
        pl.semaphore_signal(barrier, inc=1, device_id={"tp": turn(me, d, n_tp)}, device_id_type=MESH)
    for d in range(1, n_x):
        pl.semaphore_signal(barrier, inc=1, device_id={"ep": turn(ep, 2 * d, n_ep)}, device_id_type=MESH)
    pl.semaphore_signal(barrier, inc=1, device_id={"ep": partner}, device_id_type=MESH)
    pl.semaphore_wait(barrier, n_tp + n_x - 1)
    for cp in start:
        cp.wait()
    loads = []
    for i, (src, dst) in enumerate(((sg, vg), (su, vu), (sd, vd))):
        cp = pltpu.make_async_copy(src, dst, vsem.at[i])
        cp.start()
        loads.append(cp)
    for e in range(n_exp):
        for i, (src, dst) in enumerate(((eg, wg), (eu, wu), (ed, wd))):
            pltpu.make_async_copy(src.at[e], dst.at[e], wsem.at[i, e]).start()


    total, pend = rows_reduce(part, (relay0, recv0), (s1, r1), me, n_tp, rows)
    y = (resid[...].astype(F32) + total).astype(BF16)
    y_own[...] = y
    xs[ep, me] = rms_norm(y, gain[1:2, :])

    order = [2, 1, 3, 0]
    source = [turn(ep, n_ep - 2 * k, n_ep) for k in range(n_x)]
    xcp, ycp, zcp, pcp = {}, {}, {}, {}
    for k in order[:-1]:
        xcp[k] = remote(xs.at[ep, me], xs.at[ep, me], sx.at[k - 1], rx.at[k - 1], {"ep": turn(ep, 2 * k, n_ep)})
        xcp[k].start()
    far = turn(me, 2, n_tp)
    for k in [0] + order[:-1]:
        if k:
            xcp[k].wait_recv()
        mine = xs.at[source[k], me]
        for i, peer in enumerate((up, down, far) if k == order[0] else (up, down)):
            ycp[k, i] = remote(mine, mine, sy.at[k, i], ry.at[k, i], {"tp": peer})
            ycp[k, i].start()

    def forward(k):
        for i, (origin, peer, part_of) in enumerate(((down, up, lo), (up, down, hi))):
            ycp[k, i].wait_recv()
            piece = xs.at[source[k], origin, :, part_of]
            zcp[k, i] = remote(piece, piece, sz.at[k, i], rz.at[k, i], {"tp": peer})
            zcp[k, i].start()

    def across(k):
        for i in range(2 if k != order[0] else 3):
            (zcp if k != order[0] else ycp)[k, i].wait_recv()
        pcp[k] = remote(xs.at[source[k]], xs.at[source[k]], sd2.at[k], rd2.at[k], {"ep": partner})
        pcp[k].start()

    acc[...] = jnp.zeros(acc.shape, F32)
    forward(0)
    across(0)
    for cp in loads:
        cp.wait()
    own = xs[ep].reshape(block, hidden)
    shbuf[...] = nn(silu_mul(nt(own, vg[...]), nt(own, vu[...])), vd[...])
    across(order[0])

    def weights(at, x, xb):
        logits = nt(x, router[...])
        ex = jnp.exp(logits - jnp.max(logits, axis=-1, keepdims=True))
        prob = ex / jnp.sum(ex, axis=-1, keepdims=True)
        lane = lax.broadcasted_iota(jnp.int32, prob.shape, 1)
        picks = ids[pl.ds(2 * xb, 2)].reshape(2 * block, ids.shape[-1])
        chosen = lane == picks[:, 0:1]
        for j in range(1, top_k):
            chosen = chosen | (lane == picks[:, j:j + 1])
        comb[at] = jnp.where(chosen, prob, 0.0)

    half = hidden // 2
    pieces = (lo, hi)

    def gate_up(xk, e, first=False):
        if first:
            for i, (src, dst) in enumerate(((eg, wg), (eu, wu), (ed, wd))):
                pltpu.make_async_copy(src.at[e], dst.at[e], wsem.at[i, e]).wait()
        return jnp.transpose(jax.nn.silu(nt(wg[e], xk)) * nt(wu[e], xk)).astype(BF16)

    def add_down(act, e, at, count, piece):
        n = 2 * block * count
        cw = comb[at:at + count].reshape(n, comb.shape[-1])
        lane = lax.broadcasted_iota(jnp.int32, cw.shape, 1)
        col = jnp.sum(jnp.where(lane == ep * n_exp + e, cw, 0.0), axis=-1, keepdims=True)
        for q in range(2):
            cs = pl.ds(piece * half + q * (half // 2), half // 2)
            acc[at:at + count, :, cs] += (col * nn(act, wd[e, :, cs])).reshape(count, 2 * block, half // 2)

    def experts(load, at, lo_e, hi_e, first=False):
        def body(e, _):
            act = gate_up(load(), e, first)
            for piece in range(2):
                add_down(act, e, at, 1, piece)
            return 0
        lax.fori_loop(lo_e, hi_e, body, 0)

    def pair_acts(lo_e, hi_e):
        def body(e, _):
            acts[e] = gate_up(xpair[...], e)
            return 0
        lax.fori_loop(lo_e, hi_e, body, 0)

    def pair_down(piece, lo_e, hi_e):
        def body(e, _):
            add_down(acts[e], e, 1, 2, piece)
            return 0
        lax.fori_loop(lo_e, hi_e, body, 0)

    target = [turn(xi, d, n_x) for d in (2, 1, n_x - 1, 0)]
    arrive = [2, n_x - 1, 1, 0]
    kept = pl.ds(core * block, block)
    other = pl.ds((1 - core) * block, block)
    dcp, acp = {}, {}

    def ready(b):
        pcp[arrive[b]].wait_recv()

    def cross(b, piece):
        cs = pieces[piece]
        dcp[b, piece] = remote(acc.at[b, other, cs], drecv.at[b, :, cs], sb.at[b, piece], rb.at[b, piece], {"ep": partner})
        dcp[b, piece].start()

    def along(src, dst, i, d):
        acp[i] = remote(src, dst, sa.at[i], ra.at[i], {"ep": turn(ep, 2 * d, n_ep)})
        acp[i].start()

    def settle(b, piece):
        cs = pieces[piece]
        dcp[b, piece].wait_recv()
        drecv[b, :, cs] = drecv[b, :, cs] + acc[b, kept, cs]

    def pass_on(piece):
        for b, d in ((1, 1), (2, n_x - 1)):
            cs = pieces[piece]
            settle(b, piece)
            if b == piece + 1:
                acp[piece].wait_recv()
                drecv[b, :, cs] = drecv[b, :, cs] + xrelay[piece]
            along(drecv.at[b, :, cs], xrecv.at[b - 1, :, cs], 2 * b + piece, d)

    ready(0)
    far_rows = lambda: xs[pl.ds(2 * target[0], 2)].reshape(2 * block, hidden)
    weights(0, far_rows(), target[0])
    experts(far_rows, 0, 0, 2, True)
    forward(1)
    forward(3)
    experts(far_rows, 0, 2, 5, True)
    across(1)
    across(3)
    experts(far_rows, 0, 5, n_exp, True)
    for piece in range(2):
        cross(0, piece)
    for b in (1, 2):
        ready(b)
        xb = xs[pl.ds(2 * target[b], 2)].reshape(2 * block, hidden)
        xpair[(b - 1) * 2 * block:b * 2 * block, :] = xb
        weights(b, xb, target[b])
    pair_acts(0, 1)
    for piece in range(2):
        settle(0, piece)
        along(drecv.at[0, :, pieces[piece]], xrelay.at[piece], piece, (1, n_x - 1)[piece])
    pair_acts(1, n_exp)
    pair_down(0, 0, n_exp)
    for b in (1, 2):
        cross(b, 0)
    pair_down(1, 0, n_exp // 2)
    pass_on(0)
    pair_down(1, n_exp // 2, n_exp)
    for b in (1, 2):
        cross(b, 1)
    ready(3)
    own_rows = lambda: xs[pl.ds(2 * target[3], 2)].reshape(2 * block, hidden)
    weights(3, own_rows(), target[3])
    experts(own_rows, 3, 0, 2)
    pass_on(1)
    experts(own_rows, 3, 2, n_exp)
    for piece in range(2):
        cross(3, piece)
    for piece in range(2):
        settle(3, piece)
    for i in range(2, 6):
        acp[i].wait_recv()
    drecv[3] = drecv[3] + shbuf[...] + (xrecv[0] + xrecv[1])
    total, last = rows_reduce(drecv.at[3], (relay1, recv1), (sc, rc), me, n_tp, rows)
    fin = (y_own[...].astype(F32) + total).astype(BF16)
    obuf[me] = fin
    ocp = rows_gather(obuf, so, ro, me, n_tp)
    out[pl.ds(me * rows, rows), :] = fin
    for d in range(1, n_tp):
        ocp[d - 1].wait_recv()
        src = turn(me, n_tp - d, n_tp)
        out[pl.ds(src * rows, rows), :] = obuf[src]
    pend = pend + list(xcp.values()) + list(ycp.values()) + list(zcp.values()) + list(pcp.values())
    for cp in pend + list(dcp.values()) + list(acp.values()) + last + ocp:
        cp.wait_send()


def moe(n_tp, n_ep, top_k, part, resid, gain, router, ids, sg, su, sd, eg, eu, ed):
    rows, hidden = part.shape
    own = rows // n_tp
    n_x = n_ep // 2
    dma = pltpu.SemaphoreType.DMA
    n_exp = eg.shape[0]
    vm = pl.BlockSpec(memory_space=pltpu.VMEM)
    hbm = pl.BlockSpec(memory_space=pl.ANY)
    first = (part, resid, gain, router, ids)
    scratch = [
        *[pltpu.VMEM(v.shape, v.dtype) for v in first], dma((len(first),)),
        pltpu.VMEM(eg.shape, BF16), pltpu.VMEM(eu.shape, BF16), pltpu.VMEM(ed.shape, BF16),
        pltpu.VMEM(sg.shape, BF16), pltpu.VMEM(su.shape, BF16), pltpu.VMEM(sd.shape, BF16),
        pltpu.VMEM((n_ep, n_tp, own, hidden), BF16),
        pltpu.VMEM((own, hidden), BF16),
        *reduce_scratch(own, hidden),
        pltpu.VMEM((n_x, 2 * rows, router.shape[0]), F32),
        pltpu.VMEM((n_x, 2 * rows, hidden), F32),
        pltpu.VMEM((n_x, rows, hidden), F32),
        pltpu.VMEM((2, rows, hidden // 2), F32),
        pltpu.VMEM((2, rows, hidden), F32),
        pltpu.VMEM((rows, hidden), F32),
        pltpu.VMEM((4 * rows, hidden), BF16),
        pltpu.VMEM((n_exp, 4 * rows, eg.shape[1]), BF16),
        *reduce_scratch(own, hidden),
        pltpu.VMEM((n_tp, own, hidden), BF16),
        dma((3, n_exp)), dma((3,)),
        *[dma((6,))] * 2, *[dma((n_x - 1,))] * 2, *[dma((n_x, 3))] * 2, *[dma((n_x, 2))] * 2, *[dma((n_x,))] * 2,
        *[dma((6,))] * 2, *[dma((n_x, 2))] * 2, *[dma((6,))] * 2,
        dma((n_tp - 1,)), dma((n_tp - 1,)),
    ]
    return pl.pallas_call(
        functools.partial(moe_kernel, n_tp, n_ep, top_k),
        out_shape=jax.ShapeDtypeStruct((rows, hidden), BF16),
        in_specs=[hbm] * 11,
        out_specs=vm,
        scratch_shapes=scratch,
        compiler_params=pltpu.CompilerParams(collective_id=2, has_side_effects=True, vmem_limit_bytes=VMEM_ALL),
        name="moe",
    )(*first, sg, su, sd, eg, eu, ed)


def solution(mesh):
    tok_axes = ('dp', 'ep')
    n_tp, n_ep = mesh.shape['tp'], mesh.shape['ep']

    def device_fn(emb, pos, route_ids, lat_cache, rope_cache, attn_norm, w_q, w_dkv, kv_norm, w_uk, w_uv, w_o, mlp_norm, dense_gate, dense_up, dense_down, router, shared_gate, shared_up, shared_down, expert_gate, expert_up, expert_down):
        steps, tokens, hidden = emb.shape
        rows = steps * tokens
        emb_rows = emb.reshape(rows, hidden)
        ids = route_ids.transpose(2, 0, 1)
        rope_dim = rope_cache.shape[-1]
        inv_freq = np.float32(ROPE_THETA) ** (-(np.arange(rope_dim // 2, dtype=np.float32) * np.float32(2.0) / np.float32(rope_dim)))
        freq = jnp.asarray(np.concatenate([inv_freq, inv_freq])[:, None])
        layers = w_q.shape[0]
        wq_t = w_q.transpose(0, 2, 3, 1)
        wdkv_t = w_dkv.swapaxes(1, 2)
        rop_t = rope_cache.swapaxes(2, 3)
        wuk = w_uk.reshape(layers, -1, w_uk.shape[-1])
        wuv = w_uv.reshape(layers, -1, w_uv.shape[-1])

        def attend(layer, x, outs):
            return attention(layer, steps, x, attn_norm, pos, freq, kv_norm, wq_t, wdkv_t, wuk, wuv, w_o, lat_cache, rop_t, outs)

        part, *outs = attend(0, emb_rows, None)
        h_own, normed, ids_all = mid(n_tp, n_ep, part, emb_rows, mlp_norm, attn_norm, ids, dense_gate.T, dense_up.T, dense_down)
        part, lat_out, rop_out = attend(1, normed, outs)
        out = moe(n_tp, n_ep, route_ids.shape[-1], part, h_own, mlp_norm, router.T, ids_all, shared_gate.T, shared_up.T, shared_down, expert_gate.swapaxes(1, 2), expert_up.swapaxes(1, 2), expert_down)
        return out.reshape(steps, tokens, hidden), lat_out, rop_out.swapaxes(2, 3)

    tok, wide, tall = P(None, tok_axes), P(None, 'tp'), P('tp')
    heads = P(None, None, 'tp')
    in_specs = (tok, P(tok_axes), tok, tok, tok, P(), heads, P(), P(), heads, heads, wide, P(), wide, wide, tall, P(), wide, wide, tall, P('ep', None, 'tp'), P('ep', None, 'tp'), P('ep', 'tp'))
    out_specs = (tok, tok, tok)
    return jax.shard_map(device_fn, mesh=mesh, in_specs=in_specs, out_specs=out_specs, check_vma=False)
```

```python
import functools
import math
import jax
import jax.numpy as jnp
import numpy as np
from jax import lax
from jax.experimental import pallas as pl
from jax.experimental.pallas import tpu as pltpu
from jax.sharding import PartitionSpec as P

NORM_EPS = 1e-6
ROPE_THETA = 10000.0
MESH = pl.DeviceIdType.MESH
F32 = jnp.float32
BF16 = jnp.bfloat16
VMEM_ALL = 67043328


def rms_norm(values, gain):
    wide = values.astype(F32)
    mean_sq = jnp.mean(wide * wide, axis=-1, keepdims=True)
    return (wide * lax.rsqrt(mean_sq + NORM_EPS) * gain).astype(BF16)


def nt(a, b):
    return lax.dot_general(a, b, (((1,), (1,)), ((), ())), preferred_element_type=F32)


def nn(a, b):
    return jnp.dot(a, b, preferred_element_type=F32)


def silu_mul(gate, up):
    return (jax.nn.silu(gate) * up).astype(BF16)


def attn_kernel(layer, steps, group, *refs):
    n_in = 13 if layer == 0 else 15
    (x, gain, pos, pos_row, freq, g_kv, wq, wdkv, wuk, wuv, wo, lat, rop) = refs[:13]
    part, lat_out, rop_out = refs[n_in:n_in + 3]
    (wqb, wdkvb, wukb, wuvb, wob, latb, ropb, qls, qrs, latn, ropn, outs, wide,
     wsem, csem, osem) = refs[n_in + 3:]
    lora = g_kv.shape[1]
    tok = latb.shape[0]
    cache = latb.shape[1]
    rope = ropb.shape[1]
    half = rope // 2
    heads = outs.shape[1] // (steps * tok)
    qk = wqb.shape[0] // heads
    nope = qk - rope
    scale = 1.0 / math.sqrt(qk)
    per = steps * heads
    n_group = tok // group

    loads = []
    for i, (src, dst) in enumerate(((wq, wqb), (wdkv, wdkvb), (wuk, wukb), (wuv, wuvb), (wo, wob))):
        loads.append(pltpu.make_async_copy(src.at[layer], dst, wsem.at[i]))

    def cache_in(g):
        t = pl.ds(g * group, group)
        return (pltpu.make_async_copy(lat.at[layer, t], latb.at[t], csem.at[0, g]),
                pltpu.make_async_copy(rop.at[layer, t], ropb.at[t], csem.at[1, g]))

    def cache_out(g):
        t = pl.ds(g * group, group)
        return (pltpu.make_async_copy(latb.at[t], lat_out.at[layer, t], osem.at[0, g]),
                pltpu.make_async_copy(ropb.at[t], rop_out.at[layer, t], osem.at[1, g]))

    for cp in loads[:3]:
        cp.start()

    places = jnp.concatenate([pos_row[...] + s for s in range(steps)], axis=1).astype(F32)
    angle = freq[...] * places
    cos_t, sin_t = jnp.cos(angle), jnp.sin(angle)
    first = lax.broadcasted_iota(jnp.int32, angle.shape, 0) < half
    cosf, sinf = jnp.transpose(cos_t), jnp.transpose(jnp.where(first, -sin_t, sin_t))
    cost, sint = cos_t[:half], sin_t[:half]

    normed = rms_norm(x[...], gain[layer:layer + 1, :]) if layer == 0 else x[...]
    loads[0].wait()
    for g in range(n_group):
        for cp in cache_in(g):
            cp.start()
    for cp in loads[3:]:
        cp.start()
    query = nt(normed, wqb[...])
    loads[1].wait()
    kv = nt(normed, wdkvb[:lora, :])
    latn[...] = rms_norm(kv, g_kv[layer:layer + 1, :]).astype(F32)
    key = nt(wdkvb[lora:, :], normed)
    k1, k2 = key[:half], key[half:]
    ropn[...] = jnp.concatenate([k1 * cost - k2 * sint, k2 * cost + k1 * sint], axis=0).astype(BF16).astype(F32)
    loads[2].wait()
    wide[...] = wukb[...].astype(F32)
    for h in range(heads):
        base = h * qk
        qn = query[:, base:base + nope].astype(BF16)
        pe = query[:, base + nope:base + qk]
        swapped = jnp.concatenate([pe[:, half:], pe[:, :half]], axis=1)
        turned = pe * cosf + swapped * sinf
        ql = nt(qn, wide[pl.ds(h, lora, stride=heads), :].astype(BF16))
        for s in range(steps):
            at = slice((s * heads + h) * tok, (s * heads + h + 1) * tok)
            qrs[at, :rope] = turned[s * tok:(s + 1) * tok]
            for c in range(lora // 128):
                qls[c, at, :] = ql[s * tok:(s + 1) * tok, c * 128:(c + 1) * 128]

    row16 = lax.broadcasted_iota(jnp.int32, (16, lora), 0)
    lane_c = lax.broadcasted_iota(jnp.int32, (rope, cache), 1)
    lane_r = lax.broadcasted_iota(jnp.int32, (rope, steps * tok), 1)
    lane_s = lax.broadcasted_iota(jnp.int32, (per, cache), 1)
    step_s = lax.broadcasted_iota(jnp.int32, (per, cache), 0) // heads

    def run_group(g, _):
        for cp in cache_in(g):
            cp.wait()
        for j in range(group):
            b = g * group + j
            p = pos[b]
            rb = ropb[b].astype(F32)
            for s in range(steps):
                slot = p + s
                start = pl.multiple_of((slot // 16) * 16, 16)
                old = latb[b, pl.ds(start, 16), :].astype(F32)
                new = latn[pl.ds(s * tok + b, 1), :]
                latb[b, pl.ds(start, 16), :] = jnp.where(row16 == slot - start, new, old).astype(BF16)
                col = jnp.sum(jnp.where(lane_r == s * tok + b, ropn[...], 0.0), axis=1, keepdims=True)
                rb = jnp.where(lane_c == slot, col, rb)
            ropb[b] = rb.astype(BF16)
        for cp in cache_out(g):
            cp.start()
        probs = []
        for j in range(group):
            b = g * group + j
            mine = pl.ds(b, per, stride=tok)
            ql = jnp.concatenate([qls[c, mine, :] for c in range(lora // 128)], axis=1).astype(BF16)
            qr = qrs[mine, :][:, :rope].astype(BF16)
            sc = (nt(ql, latb[b]) + nn(qr, ropb[b])) * scale
            sc = jnp.where(lane_s <= pos[b] + step_s, sc, -1e30)
            ex = jnp.exp(sc - jnp.max(sc, axis=-1, keepdims=True))
            probs.append((ex / jnp.sum(ex, axis=-1, keepdims=True)).astype(BF16))
        for j in range(group):
            b = g * group + j
            val = nn(probs[j], latb[b])
            for c in range(lora // 128):
                outs[c, pl.ds(b, per, stride=tok), :] = val[:, c * 128:(c + 1) * 128]
        return 0

    lax.fori_loop(0, n_group, run_group, 0)
    loads[3].wait()
    wide[...] = wuvb[...].astype(F32)
    vals = []
    for h in range(heads):
        ol = jnp.concatenate([
            jnp.concatenate([outs[c, (s * heads + h) * tok:(s * heads + h + 1) * tok, :] for s in range(steps)], axis=0)
            for c in range(lora // 128)], axis=1).astype(BF16)
        vals.append(nn(ol, wide[pl.ds(h, lora, stride=heads), :].astype(BF16)).astype(BF16))
    loads[4].wait()
    part[...] = nn(jnp.concatenate(vals, axis=1), wob[...])
    for g in range(n_group):
        for cp in cache_out(g):
            cp.wait()


def attention(layer, steps, x, gain, pos, freq, g_kv, wq, wdkv, wuk, wuv, wo, lat, rop, outs):
    rows = x.shape[0]
    tok, cache, lora = lat.shape[1:]
    rope = rop.shape[2]
    hidden = wo.shape[2]
    heads = wq.shape[1]
    qk = wq.shape[2]
    group = 8
    vm = pl.BlockSpec(memory_space=pltpu.VMEM)
    hbm = pl.BlockSpec(memory_space=pl.ANY)
    sm = pl.BlockSpec(memory_space=pltpu.SMEM)
    wq2 = wq.reshape(wq.shape[0], heads * qk, -1)
    args = [x, gain, pos, pos[None, :], freq, g_kv, wq2, wdkv, wuk, wuv, wo, lat, rop]
    specs = [vm, vm, sm] + [vm] * 3 + [hbm] * 7
    alias = {}
    if outs is not None:
        args += list(outs)
        specs += [hbm, hbm]
        alias = {13: 1, 14: 2}
    dma = pltpu.SemaphoreType.DMA
    return pl.pallas_call(
        functools.partial(attn_kernel, layer, steps, group),
        out_shape=[jax.ShapeDtypeStruct((rows, hidden), F32),
                   jax.ShapeDtypeStruct(lat.shape, BF16), jax.ShapeDtypeStruct(rop.shape, BF16)],
        in_specs=specs,
        out_specs=[vm, hbm, hbm],
        input_output_aliases=alias,
        scratch_shapes=[
            pltpu.VMEM(wq2.shape[1:], BF16), pltpu.VMEM(wdkv.shape[1:], BF16), pltpu.VMEM(wuk.shape[1:], BF16),
            pltpu.VMEM(wuv.shape[1:], BF16), pltpu.VMEM(wo.shape[1:], BF16),
            pltpu.VMEM((tok, cache, lora), BF16), pltpu.VMEM((tok, rope, cache), BF16),
            pltpu.VMEM((lora // 128, rows * heads, 128), F32), pltpu.VMEM((rows * heads, 128), F32),
            pltpu.VMEM((rows, lora), F32), pltpu.VMEM((rope, rows), F32), pltpu.VMEM((lora // 128, rows * heads, 128), F32),
            pltpu.VMEM(wuk.shape[1:], F32),
            dma((5,)), dma((2, tok // group)), dma((2, tok // group)),
        ],
        compiler_params=pltpu.CompilerParams(vmem_limit_bytes=VMEM_ALL),
        name="attn%d" % layer,
    )(*args)


def remote(src, dst, send, recv, where):
    return pltpu.make_async_remote_copy(src_ref=src, dst_ref=dst, send_sem=send, recv_sem=recv,
                                        device_id=where, device_id_type=MESH)


def turn(me, d, n):
    return lax.rem(me + d, n)


def fetch(refs, sem):
    half = len(refs) // 2
    cps = [pltpu.make_async_copy(src, dst, sem.at[i]) for i, (src, dst) in enumerate(zip(refs[:half], refs[half:]))]
    for cp in cps:
        cp.start()
    return cps, refs[half:]


def rows_reduce(part, bufs, sems, me, n_tp, rows):
    relay, fin = bufs
    hidden = part.shape[1]
    lo, hi = pl.ds(0, hidden // 2), pl.ds(hidden // 2, hidden // 2)
    up, far, down = turn(me, 1, n_tp), turn(me, 2, n_tp), turn(me, n_tp - 1, n_tp)

    def at(owner):
        return pl.ds(owner * rows, rows)

    def send(src, dst, i, peer):
        cp = remote(src, dst, sems[0].at[i], sems[1].at[i], {"tp": peer})
        cp.start()
        return cp

    cps = [send(part.at[at(far), lo], relay.at[0], 0, up), send(part.at[at(far), hi], relay.at[1], 1, down),
           send(part.at[at(up), hi], fin.at[0, :, hi], 2, up), send(part.at[at(down), lo], fin.at[1, :, lo], 3, down)]
    cps[0].wait_recv()
    relay[0] = relay[0] + part[at(up), lo]
    cps.append(send(relay.at[0], fin.at[0, :, lo], 4, up))
    cps[1].wait_recv()
    relay[1] = relay[1] + part[at(down), hi]
    cps.append(send(relay.at[1], fin.at[1, :, hi], 5, down))
    for cp in cps[2:]:
        cp.wait_recv()
    return part[at(me), :] + (fin[0] + fin[1]), cps


def reduce_scratch(own, hidden):
    return [pltpu.VMEM((2, own, hidden // 2), F32), pltpu.VMEM((2, own, hidden), F32)]


def rows_gather(buf, s, r, me, n_tp):
    cps = [remote(buf.at[me], buf.at[me], s.at[d - 1], r.at[d - 1], {"tp": turn(me, d, n_tp)}) for d in range(1, n_tp)]
    for cp in cps[1:] + cps[:1]:
        cp.start()
    return cps


def mid_kernel(n_tp, n_ep, step, part_in, resid_in, gain0_in, gain1_in, ids_in, wg, wu, wd,
               own_out, norm_out, ids_out, part, resid, gain0, gain1, ids, in_sem,
               wgb, wub, wdb, relay0, recv0, relay1, recv1, gath0, gath1, acc, ids_own, ids_all,
               wsem, s1, r1, s2, r2, s3, r3, s4, r4, s5, r5):
    me = lax.axis_index("tp")
    ep = lax.axis_index("ep")
    total_rows, hidden = part.shape
    rows = total_rows // n_tp
    first, _ = fetch((part_in, resid_in, gain0_in, gain1_in, ids_in, part, resid, gain0, gain1, ids), in_sem)
    barrier = pltpu.get_barrier_semaphore()
    for d in range(1, n_tp):
        pl.semaphore_signal(barrier, inc=1, device_id={"tp": turn(me, d, n_tp)}, device_id_type=MESH)
    for d in range(1, n_ep):
        pl.semaphore_signal(barrier, inc=1, device_id={"ep": turn(ep, d, n_ep)}, device_id_type=MESH)
    pl.semaphore_wait(barrier, n_tp - 1 + n_ep - 1)
    for cp in first:
        cp.wait()
    loads = []
    for i, (src, dst) in enumerate(((wg, wgb), (wu, wub), (wd, wdb))):
        cp = pltpu.make_async_copy(src, dst, wsem.at[i])
        cp.start()
        loads.append(cp)

    id_cps = []
    picks = jnp.concatenate([ids[:, i, :] for i in range(ids.shape[1])], axis=1).astype(F32)
    picks = jnp.concatenate([picks, jnp.zeros((8 - picks.shape[0], picks.shape[1]), F32)], axis=0)
    ids_own[...] = jnp.zeros(ids_own.shape, jnp.int32)
    ids_own[:, 0:8] = jnp.transpose(picks).astype(jnp.int32)
    for d in range(1, n_ep):
        cp = remote(ids_own, ids_all.at[ep], s5.at[d - 1], r5.at[d - 1], {"ep": turn(ep, d, n_ep)})
        cp.start()
        id_cps.append(cp)
    ids_out[ep] = ids_own[...]
    own = pl.ds(me * rows, rows)
    total, red0 = rows_reduce(part, (relay0, recv0), (s1, r1), me, n_tp, rows)
    y = (resid[own, :].astype(F32) + total).astype(BF16)
    gath0[me] = rms_norm(y, gain0[0:1, :])
    gat0 = rows_gather(gath0, s2, r2, me, n_tp)
    for cp in loads:
        cp.wait()
    for cp in gat0:
        cp.wait_recv()

    width = wgb.shape[0]

    def chunk(start, size, first):
        x = gath0[...].reshape(total_rows, hidden)
        act = silu_mul(nt(x, wgb[pl.ds(start, size), :]), nt(x, wub[pl.ds(start, size), :]))
        down = nn(act, wdb[pl.ds(start, size), :])
        acc[...] = down if first else acc[...] + down

    whole = width // step
    chunk(0, step, True)

    def body(i, _):
        chunk(pl.multiple_of(i * step, step), step, False)
        return 0

    lax.fori_loop(1, whole, body, 0)
    if width % step:
        chunk(whole * step, width % step, False)

    total, red1 = rows_reduce(acc, (relay1, recv1), (s3, r3), me, n_tp, rows)
    h = (y.astype(F32) + total).astype(BF16)
    own_out[...] = h
    normed = rms_norm(h, gain1[1:2, :])
    gath1[me] = normed
    gat1 = rows_gather(gath1, s4, r4, me, n_tp)
    norm_out[own, :] = normed
    for d in range(1, n_ep):
        id_cps[d - 1].wait_recv()
        src = turn(ep, n_ep - d, n_ep)
        ids_out[src] = ids_all[src]
    for d in range(1, n_tp):
        gat1[d - 1].wait_recv()
        src = turn(me, n_tp - d, n_tp)
        norm_out[pl.ds(src * rows, rows), :] = gath1[src]
    for cp in red0 + gat0 + red1 + gat1 + id_cps:
        cp.wait_send()


def mid(n_tp, n_ep, part, resid, gain0, gain1, ids, wg, wu, wd):
    rows, hidden = part.shape
    first = (part, resid, gain0, gain1, ids)
    own = rows // n_tp
    dma = pltpu.SemaphoreType.DMA
    vm = pl.BlockSpec(memory_space=pltpu.VMEM)
    hbm = pl.BlockSpec(memory_space=pl.ANY)
    return pl.pallas_call(
        functools.partial(mid_kernel, n_tp, n_ep, 512),
        out_shape=[jax.ShapeDtypeStruct((own, hidden), BF16), jax.ShapeDtypeStruct((rows, hidden), BF16),
                   jax.ShapeDtypeStruct((n_ep, rows, 128), ids.dtype)],
        in_specs=[hbm] * 8,
        out_specs=[vm] * 3,
        scratch_shapes=[
            *[pltpu.VMEM(v.shape, v.dtype) for v in first], dma((len(first),)),
            pltpu.VMEM(wg.shape, BF16), pltpu.VMEM(wu.shape, BF16), pltpu.VMEM(wd.shape, BF16),
            *reduce_scratch(own, hidden), *reduce_scratch(own, hidden),
            pltpu.VMEM((n_tp, own, hidden), BF16), pltpu.VMEM((n_tp, own, hidden), BF16),
            pltpu.VMEM((rows, hidden), F32), pltpu.VMEM((rows, 128), ids.dtype), pltpu.VMEM((n_ep, rows, 128), ids.dtype),
            dma((3,))] + [dma((6,)), dma((6,)), dma((n_tp - 1,)), dma((n_tp - 1,))] * 2 + [dma((n_ep - 1,))] * 2,
        compiler_params=pltpu.CompilerParams(collective_id=0, has_side_effects=True, vmem_limit_bytes=VMEM_ALL),
        name="mid",
    )(*first, wg, wu, wd)


def moe_kernel(n_tp, n_ep, top_k, part_in, resid_in, gain_in, router_in, ids_in, sg, su, sd, eg, eu, ed, out,
               part, resid, gain, router, ids, in_sem,
               wg, wu, wd, vg, vu, vd, xs, y_own, relay0, recv0, comb, acc, drecv, xrelay, xrecv, shbuf, xpair, acts,
               relay1, recv1, obuf,
               wsem, vsem, s1, r1, sx, rx, sy, ry, sz, rz, sd2, rd2, sa, ra, sb, rb, sc, rc, so, ro):
    me = lax.axis_index("tp")
    ep = lax.axis_index("ep")
    xi, core = ep // 2, lax.rem(ep, 2)
    n_x = n_ep // 2
    partner = ep + 1 - 2 * core
    rows = part.shape[0] // n_tp
    hidden = part.shape[1]
    block = part.shape[0]
    n_exp = wg.shape[0]
    lo, hi = pl.ds(0, hidden // 2), pl.ds(hidden // 2, hidden // 2)
    up, down = turn(me, 1, n_tp), turn(me, n_tp - 1, n_tp)

    start, _ = fetch((part_in, resid_in, gain_in, router_in, ids_in, part, resid, gain, router, ids), in_sem)
    barrier = pltpu.get_barrier_semaphore()
    for d in range(1, n_tp):
        pl.semaphore_signal(barrier, inc=1, device_id={"tp": turn(me, d, n_tp)}, device_id_type=MESH)
    for d in range(1, n_x):
        pl.semaphore_signal(barrier, inc=1, device_id={"ep": turn(ep, 2 * d, n_ep)}, device_id_type=MESH)
    pl.semaphore_signal(barrier, inc=1, device_id={"ep": partner}, device_id_type=MESH)
    pl.semaphore_wait(barrier, n_tp + n_x - 1)
    for cp in start:
        cp.wait()
    loads = []
    for i, (src, dst) in enumerate(((sg, vg), (su, vu), (sd, vd))):
        cp = pltpu.make_async_copy(src, dst, vsem.at[i])
        cp.start()
        loads.append(cp)
    for e in range(n_exp):
        for i, (src, dst) in enumerate(((eg, wg), (eu, wu), (ed, wd))):
            pltpu.make_async_copy(src.at[e], dst.at[e], wsem.at[i, e]).start()


    total, pend = rows_reduce(part, (relay0, recv0), (s1, r1), me, n_tp, rows)
    y = (resid[...].astype(F32) + total).astype(BF16)
    y_own[...] = y
    xs[ep, me] = rms_norm(y, gain[1:2, :])

    order = [2, 1, 3, 0]
    source = [turn(ep, n_ep - 2 * k, n_ep) for k in range(n_x)]
    xcp, ycp, zcp, pcp = {}, {}, {}, {}
    for k in order[:-1]:
        xcp[k] = remote(xs.at[ep, me], xs.at[ep, me], sx.at[k - 1], rx.at[k - 1], {"ep": turn(ep, 2 * k, n_ep)})
        xcp[k].start()
    far = turn(me, 2, n_tp)
    for k in [0] + order[:-1]:
        if k:
            xcp[k].wait_recv()
        mine = xs.at[source[k], me]
        for i, peer in ((2, far), (0, up), (1, down))[0 if k == order[0] else 1:]:
            ycp[k, i] = remote(mine, mine, sy.at[k, i], ry.at[k, i], {"tp": peer})
            ycp[k, i].start()

    def forward(k):
        for i, (origin, peer, part_of) in enumerate(((down, up, lo), (up, down, hi))):
            ycp[k, i].wait_recv()
            piece = xs.at[source[k], origin, :, part_of]
            zcp[k, i] = remote(piece, piece, sz.at[k, i], rz.at[k, i], {"tp": peer})
            zcp[k, i].start()

    def across(k):
        for i in range(2 if k != order[0] else 3):
            (zcp if k != order[0] else ycp)[k, i].wait_recv()
        pcp[k] = remote(xs.at[source[k]], xs.at[source[k]], sd2.at[k], rd2.at[k], {"ep": partner})
        pcp[k].start()

    acc[...] = jnp.zeros(acc.shape, F32)
    forward(0)
    across(0)
    for cp in loads:
        cp.wait()
    own = xs[ep].reshape(block, hidden)
    shbuf[...] = nn(silu_mul(nt(own, vg[...]), nt(own, vu[...])), vd[...])
    across(order[0])

    def weights(at, x, xb):
        logits = nt(x, router[...])
        ex = jnp.exp(logits - jnp.max(logits, axis=-1, keepdims=True))
        prob = ex / jnp.sum(ex, axis=-1, keepdims=True)
        lane = lax.broadcasted_iota(jnp.int32, prob.shape, 1)
        picks = ids[pl.ds(2 * xb, 2)].reshape(2 * block, ids.shape[-1])
        chosen = lane == picks[:, 0:1]
        for j in range(1, top_k):
            chosen = chosen | (lane == picks[:, j:j + 1])
        comb[at] = jnp.where(chosen, prob, 0.0)

    half = hidden // 2
    pieces = (lo, hi)

    def gate_up(xk, e, first=False):
        if first:
            for i, (src, dst) in enumerate(((eg, wg), (eu, wu), (ed, wd))):
                pltpu.make_async_copy(src.at[e], dst.at[e], wsem.at[i, e]).wait()
        return jnp.transpose(jax.nn.silu(nt(wg[e], xk)) * nt(wu[e], xk)).astype(BF16)

    def add_down(act, e, at, count, piece):
        n = 2 * block * count
        cw = comb[at:at + count].reshape(n, comb.shape[-1])
        lane = lax.broadcasted_iota(jnp.int32, cw.shape, 1)
        col = jnp.sum(jnp.where(lane == ep * n_exp + e, cw, 0.0), axis=-1, keepdims=True)
        for q in range(2):
            cs = pl.ds(piece * half + q * (half // 2), half // 2)
            acc[at:at + count, :, cs] += (col * nn(act, wd[e, :, cs])).reshape(count, 2 * block, half // 2)

    def experts(load, at, lo_e, hi_e, first=False):
        def body(e, _):
            act = gate_up(load(), e, first)
            for piece in range(2):
                add_down(act, e, at, 1, piece)
            return 0
        lax.fori_loop(lo_e, hi_e, body, 0)

    def pair_acts(lo_e, hi_e):
        def body(e, _):
            acts[e] = gate_up(xpair[...], e)
            return 0
        lax.fori_loop(lo_e, hi_e, body, 0)

    def pair_down(piece, lo_e, hi_e):
        def body(e, _):
            add_down(acts[e], e, 1, 2, piece)
            return 0
        lax.fori_loop(lo_e, hi_e, body, 0)

    target = [turn(xi, d, n_x) for d in (2, 1, n_x - 1, 0)]
    arrive = [2, n_x - 1, 1, 0]
    kept = pl.ds(core * block, block)
    other = pl.ds((1 - core) * block, block)
    dcp, acp = {}, {}

    def ready(b):
        pcp[arrive[b]].wait_recv()

    def cross(b, piece):
        cs = pieces[piece]
        dcp[b, piece] = remote(acc.at[b, other, cs], drecv.at[b, :, cs], sb.at[b, piece], rb.at[b, piece], {"ep": partner})
        dcp[b, piece].start()

    def along(src, dst, i, d):
        acp[i] = remote(src, dst, sa.at[i], ra.at[i], {"ep": turn(ep, 2 * d, n_ep)})
        acp[i].start()

    def settle(b, piece):
        cs = pieces[piece]
        dcp[b, piece].wait_recv()
        drecv[b, :, cs] = drecv[b, :, cs] + acc[b, kept, cs]

    def pass_on(piece):
        for b, d in ((1, 1), (2, n_x - 1)):
            cs = pieces[piece]
            settle(b, piece)
            if b == piece + 1:
                acp[piece].wait_recv()
                drecv[b, :, cs] = drecv[b, :, cs] + xrelay[piece]
            along(drecv.at[b, :, cs], xrecv.at[b - 1, :, cs], 2 * b + piece, d)

    ready(0)
    far_rows = lambda: xs[pl.ds(2 * target[0], 2)].reshape(2 * block, hidden)
    weights(0, far_rows(), target[0])
    experts(far_rows, 0, 0, 2, True)
    forward(1)
    forward(3)
    experts(far_rows, 0, 2, 5, True)
    across(1)
    across(3)
    experts(far_rows, 0, 5, n_exp, True)
    for piece in range(2):
        cross(0, piece)
    for b in (1, 2):
        ready(b)
        xb = xs[pl.ds(2 * target[b], 2)].reshape(2 * block, hidden)
        xpair[(b - 1) * 2 * block:b * 2 * block, :] = xb
        weights(b, xb, target[b])
    pair_acts(0, 1)
    for piece in range(2):
        settle(0, piece)
        along(drecv.at[0, :, pieces[piece]], xrelay.at[piece], piece, (1, n_x - 1)[piece])
    pair_acts(1, n_exp)
    pair_down(0, 0, n_exp)
    for b in (1, 2):
        cross(b, 0)
    pair_down(1, 0, n_exp // 2)
    pass_on(0)
    pair_down(1, n_exp // 2, n_exp)
    for b in (1, 2):
        cross(b, 1)
    ready(3)
    own_rows = lambda: xs[pl.ds(2 * target[3], 2)].reshape(2 * block, hidden)
    weights(3, own_rows(), target[3])
    experts(own_rows, 3, 0, 2)
    pass_on(1)
    experts(own_rows, 3, 2, n_exp)
    for piece in range(2):
        cross(3, piece)
    for piece in range(2):
        settle(3, piece)
    for i in range(2, 6):
        acp[i].wait_recv()
    drecv[3] = drecv[3] + shbuf[...] + (xrecv[0] + xrecv[1])
    total, last = rows_reduce(drecv.at[3], (relay1, recv1), (sc, rc), me, n_tp, rows)
    fin = (y_own[...].astype(F32) + total).astype(BF16)
    obuf[me] = fin
    ocp = rows_gather(obuf, so, ro, me, n_tp)
    out[pl.ds(me * rows, rows), :] = fin
    for d in range(1, n_tp):
        ocp[d - 1].wait_recv()
        src = turn(me, n_tp - d, n_tp)
        out[pl.ds(src * rows, rows), :] = obuf[src]
    pend = pend + list(xcp.values()) + list(ycp.values()) + list(zcp.values()) + list(pcp.values())
    for cp in pend + list(dcp.values()) + list(acp.values()) + last + ocp:
        cp.wait_send()


def moe(n_tp, n_ep, top_k, part, resid, gain, router, ids, sg, su, sd, eg, eu, ed):
    rows, hidden = part.shape
    own = rows // n_tp
    n_x = n_ep // 2
    dma = pltpu.SemaphoreType.DMA
    n_exp = eg.shape[0]
    vm = pl.BlockSpec(memory_space=pltpu.VMEM)
    hbm = pl.BlockSpec(memory_space=pl.ANY)
    first = (part, resid, gain, router, ids)
    scratch = [
        *[pltpu.VMEM(v.shape, v.dtype) for v in first], dma((len(first),)),
        pltpu.VMEM(eg.shape, BF16), pltpu.VMEM(eu.shape, BF16), pltpu.VMEM(ed.shape, BF16),
        pltpu.VMEM(sg.shape, BF16), pltpu.VMEM(su.shape, BF16), pltpu.VMEM(sd.shape, BF16),
        pltpu.VMEM((n_ep, n_tp, own, hidden), BF16),
        pltpu.VMEM((own, hidden), BF16),
        *reduce_scratch(own, hidden),
        pltpu.VMEM((n_x, 2 * rows, router.shape[0]), F32),
        pltpu.VMEM((n_x, 2 * rows, hidden), F32),
        pltpu.VMEM((n_x, rows, hidden), F32),
        pltpu.VMEM((2, rows, hidden // 2), F32),
        pltpu.VMEM((2, rows, hidden), F32),
        pltpu.VMEM((rows, hidden), F32),
        pltpu.VMEM((4 * rows, hidden), BF16),
        pltpu.VMEM((n_exp, 4 * rows, eg.shape[1]), BF16),
        *reduce_scratch(own, hidden),
        pltpu.VMEM((n_tp, own, hidden), BF16),
        dma((3, n_exp)), dma((3,)),
        *[dma((6,))] * 2, *[dma((n_x - 1,))] * 2, *[dma((n_x, 3))] * 2, *[dma((n_x, 2))] * 2, *[dma((n_x,))] * 2,
        *[dma((6,))] * 2, *[dma((n_x, 2))] * 2, *[dma((6,))] * 2,
        dma((n_tp - 1,)), dma((n_tp - 1,)),
    ]
    return pl.pallas_call(
        functools.partial(moe_kernel, n_tp, n_ep, top_k),
        out_shape=jax.ShapeDtypeStruct((rows, hidden), BF16),
        in_specs=[hbm] * 11,
        out_specs=vm,
        scratch_shapes=scratch,
        compiler_params=pltpu.CompilerParams(collective_id=2, has_side_effects=True, vmem_limit_bytes=VMEM_ALL),
        name="moe",
    )(*first, sg, su, sd, eg, eu, ed)


def solution(mesh):
    tok_axes = ('dp', 'ep')
    n_tp, n_ep = mesh.shape['tp'], mesh.shape['ep']

    def device_fn(emb, pos, route_ids, lat_cache, rope_cache, attn_norm, w_q, w_dkv, kv_norm, w_uk, w_uv, w_o, mlp_norm, dense_gate, dense_up, dense_down, router, shared_gate, shared_up, shared_down, expert_gate, expert_up, expert_down):
        steps, tokens, hidden = emb.shape
        rows = steps * tokens
        emb_rows = emb.reshape(rows, hidden)
        ids = route_ids.transpose(2, 0, 1)
        rope_dim = rope_cache.shape[-1]
        inv_freq = np.float32(ROPE_THETA) ** (-(np.arange(rope_dim // 2, dtype=np.float32) * np.float32(2.0) / np.float32(rope_dim)))
        freq = jnp.asarray(np.concatenate([inv_freq, inv_freq])[:, None])
        layers = w_q.shape[0]
        wq_t = w_q.transpose(0, 2, 3, 1)
        wdkv_t = w_dkv.swapaxes(1, 2)
        rop_t = rope_cache.swapaxes(2, 3)
        wuk = w_uk.reshape(layers, -1, w_uk.shape[-1])
        wuv = w_uv.reshape(layers, -1, w_uv.shape[-1])

        def attend(layer, x, outs):
            return attention(layer, steps, x, attn_norm, pos, freq, kv_norm, wq_t, wdkv_t, wuk, wuv, w_o, lat_cache, rop_t, outs)

        part, *outs = attend(0, emb_rows, None)
        h_own, normed, ids_all = mid(n_tp, n_ep, part, emb_rows, mlp_norm, attn_norm, ids, dense_gate.T, dense_up.T, dense_down)
        part, lat_out, rop_out = attend(1, normed, outs)
        out = moe(n_tp, n_ep, route_ids.shape[-1], part, h_own, mlp_norm, router.T, ids_all, shared_gate.T, shared_up.T, shared_down, expert_gate.swapaxes(1, 2), expert_up.swapaxes(1, 2), expert_down)
        return out.reshape(steps, tokens, hidden), lat_out, rop_out.swapaxes(2, 3)

    tok, wide, tall = P(None, tok_axes), P(None, 'tp'), P('tp')
    heads = P(None, None, 'tp')
    in_specs = (tok, P(tok_axes), tok, tok, tok, P(), heads, P(), P(), heads, heads, wide, P(), wide, wide, tall, P(), wide, wide, tall, P('ep', None, 'tp'), P('ep', None, 'tp'), P('ep', 'tp'))
    out_specs = (tok, tok, tok)
    return jax.shard_map(device_fn, mesh=mesh, in_specs=in_specs, out_specs=out_specs, check_vma=False)
```
